256 devices in a mesh: bank: 16 (over y, x), zero: 16 (over z, core).
Axes of the slice: x: 4, y: 4, z: 8, core: 2. Of those that a mesh axis runs over, the one named last changes fastest.
Arguments:
- w_down: float32 [64, 1024, 2048], P('bank', None, 'zero'), may hold values from -0.25 to 0.25
- avg_down: bfloat16 [64, 1024, 2048], P('bank', None, 'zero'), may hold values from -0.09375 to 0.09375
- router_weight: float32 [2048, 64], P('zero', 'bank'), may hold values from -0.125 to 0.125
- router_gain: float32 [2048], P('zero'), may hold values from 0.25 to 1.75
Outputs:
- serve_down: bfloat16 [64, 1024, 2048], P('bank')
- scale_down: float32 [64, 1024], P('bank')
- serve_router: bfloat16 [2048, 64], replicated
The draws below stay inside these ranges and needn't reach their ends.
All inputs are finite; a program needn't handle non-finite values.
Results may differ from the reference program's by a relative error of at most 0.001.
Values may be sent and summed in bfloat16 or wider, within the bound.
A program may use at most 128 MiB of HBM per device.

```python
import jax
import jax.numpy as jnp
from jax import lax

EXPERTS = 64
D_MODEL = 2048
D_EXPERT = 1024


def strengthened(values, key, source, target, parts, factor):
    def block_of(position):
        return (jnp.arange(values.shape[position]) // (values.shape[position] // parts)).reshape((-1,) + (1,) * (values.ndim - 1 - position))

    one_side = jax.random.permutation(key, parts)[block_of(target)]
    far = (block_of(target) + parts // 2) % parts
    return jnp.where((block_of(source) == one_side) | (block_of(source) == far), factor * values, values)


def block_levels(key, extent, shards, least, largest):
    gain, own = 1.0, jax.random.fold_in(key, 6)
    for dim, parts in shards:
        steps = jnp.exp(jax.random.uniform(jax.random.fold_in(own, dim), (parts,), jnp.float32, least / len(shards), largest / len(shards)))
        gain = gain * jnp.repeat(steps, extent[dim] // parts).reshape([-1 if axis == dim else 1 for axis in range(len(extent))])
    return gain


def scatter_about(own_key, dims, spread, limit, cuts=(), dtype=jnp.bfloat16):
    array = jax.random.normal(own_key, dims, jnp.float32) * spread
    if len(cuts) > 0:
        array = block_levels(own_key, dims, cuts, -0.22, 0.18) * array
    return jnp.clip(array, min=-limit, max=limit).astype(dtype)


def gaussian_with(rng, dims, width, bound, cuts, heavy, kind=jnp.bfloat16):
    array = width * jax.random.normal(rng, dims, jnp.float32)
    if cuts:
        array = array * block_levels(rng, dims, cuts, -0.22, 0.18)
    return jnp.clip(strengthened(array, jax.random.fold_in(rng, 3), *heavy), -bound, bound).astype(kind)


def setup_inputs(seed: int = 0) -> dict:
    key_of = jax.random.split(jax.random.key(seed), 5)
    return {
        "w_down": gaussian_with(key_of[0], (EXPERTS, D_EXPERT, D_MODEL), D_EXPERT ** -0.5, 0.25, ((0, 16), (2, 16)), (2, 1, 16, 2.0), jnp.float32),
        "avg_down": scatter_about(key_of[1], (EXPERTS, D_EXPERT, D_MODEL), (D_EXPERT * 4) ** -0.5, 0.09375, ((0, 16), (2, 16))),
        "router_weight": scatter_about(key_of[2], (D_MODEL, EXPERTS), D_MODEL ** -0.5, 0.125, ((0, 16), (1, 16)), jnp.float32),
        "router_gain": jnp.clip(1.0 + 0.15 * jax.random.normal(key_of[3], (D_MODEL,), jnp.float32), 0.25, 1.75),
    }


def reference(w_down, avg_down, router_weight, router_gain):
    fresh_down = w_down + avg_down.astype(jnp.float32)
    scale_down = jnp.sqrt(lax.optimization_barrier(jnp.sum(fresh_down * fresh_down, axis=2)))
    serve_down = (fresh_down / jnp.expand_dims(scale_down, 2)).astype(jnp.bfloat16)
    serve_router = (router_weight * router_gain[:, None]).astype(jnp.bfloat16)
    return (serve_down, scale_down, serve_router)
```

```python
import functools

import jax
import jax.numpy as jnp
from jax import lax
from jax.experimental import pallas as pl
from jax.experimental.pallas import tpu as pltpu
from jax.sharding import PartitionSpec as P

MESH = pl.DeviceIdType.MESH
SPLIT = 2


def gather_kernel(
    banks, chips, w_hbm, avg_hbm, rw_hbm, gain_hbm,
    big, scale_ref, router_ref,
    wbuf, abuf, rw_ref, gain_ref, part, other, sums, total, rblk,
    wsem, asem, osem, ssem, tsem,
    rsem_r, rsem_l, send_r, send_l, send_p, recv_p, misc_send, rz_recv, rb_recv, rp_recv,
):
    experts, rows, lanes = wbuf.shape
    bank = lax.axis_index("bank")
    zero = lax.axis_index("zero")
    z = zero // 2
    core = zero % 2
    right = ((z + 1) % chips) * 2 + core
    left = ((z + chips - 1) % chips) * 2 + core
    partner = z * 2 + (1 - core)
    half = experts // 2
    groups = rows // lanes
    piece = rows // SPLIT
    chunks = experts * SPLIT
    reach = chips // 2

    small = [pltpu.make_async_copy(rw_hbm, rw_ref, asem.at[experts]),
             pltpu.make_async_copy(gain_hbm, gain_ref, wsem.at[experts])]
    loads = []
    for e in range(experts):
        lw = pltpu.make_async_copy(w_hbm.at[e], wbuf.at[e], wsem.at[e])
        la = pltpu.make_async_copy(avg_hbm.at[e], abuf.at[e], asem.at[e])
        lw.start()
        la.start()
        loads.append((lw, la))
    for copy in small:
        copy.start()

    barrier = pltpu.get_barrier_semaphore()
    pl.semaphore_signal(barrier, inc=1, device_id={"zero": partner}, device_id_type=MESH)
    for j in range(1, chips):
        peer = ((z + j) % chips) * 2 + core
        pl.semaphore_signal(barrier, inc=1, device_id={"zero": peer}, device_id_type=MESH)
    for j in range(1, banks):
        peer = (bank + j) % banks
        pl.semaphore_signal(barrier, inc=1, device_id={"bank": peer}, device_id_type=MESH)

    eye = (
        lax.broadcasted_iota(jnp.int32, (lanes, lanes), 0)
        == lax.broadcasted_iota(jnp.int32, (lanes, lanes), 1)
    )
    for e in range(experts):
        loads[e][0].wait()
        loads[e][1].wait()
        for g in range(groups):
            at = pl.ds(g * lanes, lanes)
            fresh = wbuf[e, at, :] + abuf[e, at, :].astype(jnp.float32)
            wbuf[e, at, :] = fresh
            row = jnp.sum(fresh * fresh, axis=1, keepdims=True)
            part[e, g:g + 1, :] = jnp.sum(jnp.where(eye, row, 0.0), axis=0, keepdims=True)

    for copy in small:
        copy.wait()
    rblk[bank, zero] = rw_ref[...] * gain_ref[...]

    pl.semaphore_wait(barrier, 1 + (chips - 1) + (banks - 1))

    mine, theirs = pl.ds(core * half, half), pl.ds((1 - core) * half, half)
    swap = pltpu.make_async_remote_copy(
        part.at[theirs], other, osem.at[0], osem.at[1],
        device_id={"zero": partner}, device_id_type=MESH)
    swap.start()
    rz = []
    for j in range(1, chips):
        peer = ((z + j) % chips) * 2 + core
        rz.append(pltpu.make_async_remote_copy(
            rblk.at[bank, zero], rblk.at[bank, zero], misc_send.at[0], rz_recv,
            device_id={"zero": peer}, device_id_type=MESH))
    swap.wait()
    sums[z] = part[mine] + other[...]
    spread = []
    for j in range(1, chips):
        peer = ((z + j) % chips) * 2 + core
        spread.append(pltpu.make_async_remote_copy(
            sums.at[z], sums.at[z], ssem.at[0], ssem.at[1],
            device_id={"zero": peer}, device_id_type=MESH))
    for copy in spread:
        copy.start()
    for copy in rz:
        copy.start()
    full = pltpu.make_async_remote_copy(
        sums.at[pl.ds(0, chips - 1)], sums.at[pl.ds(0, chips - 1)], ssem.at[0], ssem.at[1],
        device_id={"zero": partner}, device_id_type=MESH)
    full.wait_recv()
    acc = sums[0]
    for k in range(1, chips):
        acc = acc + sums[k]
    total[mine] = acc
    back = pltpu.make_async_remote_copy(
        total.at[mine], total.at[mine], tsem.at[0], tsem.at[1],
        device_id={"zero": partner}, device_id_type=MESH)
    back.start()
    back.wait_recv()

    def place(k, src):
        return big.at[k // SPLIT, pl.ds((k % SPLIT) * piece, piece),
                      pl.ds(pl.multiple_of(src * lanes, lanes), lanes)]

    def to_right(slot, k, src):
        return pltpu.make_async_remote_copy(
            place(k, src), place(k, src), send_r, rsem_r.at[slot],
            device_id={"zero": right}, device_id_type=MESH)

    def to_left(slot, k, src):
        return pltpu.make_async_remote_copy(
            place(k, src), place(k, src), send_l, rsem_l.at[slot],
            device_id={"zero": left}, device_id_type=MESH)

    def to_partner(k, src):
        return pltpu.make_async_remote_copy(
            place(k, src), place(k, src), send_p, recv_p,
            device_id={"zero": partner}, device_id_type=MESH)

    columns = pl.ds(pl.multiple_of(zero * lanes, lanes), lanes)
    for e in range(experts):
        root = jnp.sqrt(total[e])
        for g in range(groups):
            scale_ref[e:e + 1, g * lanes:(g + 1) * lanes] = root[g:g + 1, :]
        for s in range(SPLIT):
            for g in range(s * groups // SPLIT, (s + 1) * groups // SPLIT):
                at = pl.ds(g * lanes, lanes)
                col = jnp.sum(jnp.where(eye, root[g:g + 1, :], 0.0), axis=1, keepdims=True)
                big[e, at, columns] = (wbuf[e, at, :] / col).astype(jnp.bfloat16)
            k = e * SPLIT + s
            to_right(k, k, zero).start()
            to_left(k, k, zero).start()
            to_partner(k, zero).start()

    def router_banks():
        pltpu.make_async_remote_copy(
            rblk.at[bank, pl.ds(0, chips - 1)], rblk.at[bank, pl.ds(0, chips - 1)], misc_send.at[0], rz_recv,
            device_id={"zero": partner}, device_id_type=MESH).wait()
        for j in range(1, banks):
            peer = (bank + j) % banks
            for q in range(chips):
                pltpu.make_async_remote_copy(
                    rblk.at[bank, 2 * q + core], rblk.at[bank, 2 * q + core], misc_send.at[1], rb_recv,
                    device_id={"bank": peer}, device_id_type=MESH).start()

    def router_partner():
        n = (banks - 1) * chips
        def all_of(ref):
            return ref.at[pl.ds(0, banks - 1), pl.ds(0, chips)]
        pltpu.make_async_remote_copy(
            all_of(rblk), all_of(rblk), misc_send.at[1], rb_recv,
            device_id={"zero": partner}, device_id_type=MESH).wait()
        for q in range(chips):
            pltpu.make_async_remote_copy(
                rblk.at[:, 2 * q + core], rblk.at[:, 2 * q + core], misc_send.at[2], rp_recv,
                device_id={"zero": partner}, device_id_type=MESH).start()

    def router_finish():
        def all_of(ref):
            return ref.at[:, pl.ds(0, chips)]
        pltpu.make_async_remote_copy(
            all_of(rblk), all_of(rblk), misc_send.at[2], rp_recv,
            device_id={"zero": partner}, device_id_type=MESH).wait()
        for b in range(banks // 4):
            for q in range(2 * chips):
                block = jnp.concatenate([rblk[4 * b + i, q] for i in range(4)], axis=0)
                n = block.shape[0]
                router_ref[b * n:(b + 1) * n, q * lanes:(q + 1) * lanes] = block.astype(jnp.bfloat16)

    slot = 0
    for d in range(1, reach + 1):
        from_left = ((z + chips - d) % chips) * 2 + core
        from_right = ((z + d) % chips) * 2 + core
        last = d == reach
        for i in range(chunks // 2 if last else chunks):
            kr = 2 * i if last else i
            kl = 2 * i + 1 if last else i
            to_right(slot, kr, from_left).wait_recv()
            if d + 1 < reach:
                to_right(slot + chunks, kr, from_left).start()
            elif d + 1 == reach and kr % 2 == 0:
                to_right(d * chunks + kr // 2, kr, from_left).start()
            to_partner(kr, from_left).start()
            to_left(slot, kl, from_right).wait_recv()
            if d + 1 < reach:
                to_left(slot + chunks, kl, from_right).start()
            elif d + 1 == reach and kl % 2 == 1:
                to_left(d * chunks + kl // 2, kl, from_right).start()
            to_partner(kl, from_right).start()
            slot += 1
        if d == 1:
            router_banks()
        if d == min(2, reach):
            router_partner()
        if d == min(3, reach):
            router_finish()

    side = pl.ds(0, chips)
    def cols(n):
        return big.at[:, :, pl.ds(0, n * lanes)]
    def wide(n):
        return big.at[pl.ds(0, experts // 2), :, pl.ds(0, n * lanes)]
    hops = wide(chips - 1)
    whole = cols(chips)
    swap_back = back
    swap_back.wait_send()
    full.wait_send()
    pltpu.make_async_remote_copy(hops, hops, send_r, rsem_r.at[0],
                                 device_id={"zero": right}, device_id_type=MESH).wait_send()
    pltpu.make_async_remote_copy(hops, hops, send_l, rsem_l.at[0],
                                 device_id={"zero": left}, device_id_type=MESH).wait_send()
    pltpu.make_async_remote_copy(whole, whole, send_p, recv_p,
                                 device_id={"zero": partner}, device_id_type=MESH).wait()


def out_kernel(big, scale, router, big_hbm, scale_hbm, router_hbm, sems):
    n = big.shape[0]
    copies = [pltpu.make_async_copy(big.at[e], big_hbm.at[e], sems.at[e]) for e in range(n)]
    copies.append(pltpu.make_async_copy(scale, scale_hbm, sems.at[n]))
    copies.append(pltpu.make_async_copy(router, router_hbm, sems.at[n + 1]))
    for copy in copies:
        copy.start()
    for copy in copies:
        copy.wait()


def solution(mesh):
    banks, zeros = mesh.shape["bank"], mesh.shape["zero"]
    chips = zeros // 2

    def shards(w_down, avg_down, router_weight, router_gain):
        experts, rows, lanes = w_down.shape
        width = lanes * zeros
        cols = router_weight.shape[1]
        vmem = pl.BlockSpec(memory_space=pltpu.VMEM)
        hbm = pl.BlockSpec(memory_space=pltpu.HBM)
        pin = lambda x: pltpu.with_memory_space_constraint(x, pltpu.HBM)
        half = experts // 2
        groups = rows // lanes
        slots = experts * SPLIT * (chips - 1) // 2
        dma = pltpu.SemaphoreType.DMA
        big, scale, router = pl.pallas_call(
            functools.partial(gather_kernel, banks, chips),
            out_shape=(
                jax.ShapeDtypeStruct((experts, rows, width), jnp.bfloat16),
                jax.ShapeDtypeStruct((experts, rows), jnp.float32),
                jax.ShapeDtypeStruct((cols * banks, width), jnp.bfloat16),
            ),
            in_specs=[hbm] * 4,
            out_specs=(vmem, vmem, vmem),
            scratch_shapes=[
                pltpu.VMEM((experts, rows, lanes), jnp.float32),
                pltpu.VMEM((experts, rows, lanes), jnp.bfloat16),
                pltpu.VMEM((cols, lanes), jnp.float32),
                pltpu.VMEM((1, lanes), jnp.float32),
                pltpu.VMEM((experts, groups, lanes), jnp.float32),
                pltpu.VMEM((half, groups, lanes), jnp.float32),
                pltpu.VMEM((chips, half, groups, lanes), jnp.float32),
                pltpu.VMEM((experts, groups, lanes), jnp.float32),
                pltpu.VMEM((banks, zeros, cols, lanes), jnp.float32),
                dma((experts + 1,)), dma((experts + 1,)), dma((2,)), dma((2,)), dma((2,)),
                dma((slots,)), dma((slots,)), dma(()), dma(()), dma(()), dma(()),
                dma((3,)), dma(()), dma(()), dma(()),
            ],
            compiler_params=pltpu.CompilerParams(
                collective_id=0, has_side_effects=True, vmem_limit_bytes=8 * 1024 * 1024),
            name="gather",
        )(pin(w_down), pin(avg_down), pin(router_weight.T), pin(router_gain.reshape(1, lanes)))
        big, scale, router = pl.pallas_call(
            out_kernel,
            out_shape=(
                jax.ShapeDtypeStruct(big.shape, big.dtype),
                jax.ShapeDtypeStruct(scale.shape, scale.dtype),
                jax.ShapeDtypeStruct(router.shape, router.dtype),
            ),
            in_specs=[vmem, vmem, vmem],
            out_specs=(hbm, hbm, hbm),
            scratch_shapes=[dma((experts + 2,))],
            compiler_params=pltpu.CompilerParams(vmem_limit_bytes=4 * 1024 * 1024),
            name="put_out",
        )(big, scale, router)
        return big, scale, router.T

    return jax.shard_map(
        shards,
        mesh=mesh,
        in_specs=(P("bank", None, "zero"), P("bank", None, "zero"), P("zero", "bank"), P("zero")),
        out_specs=(P("bank", None, None), P("bank", None), P()),
        check_vma=False,
    )
```

```python
import functools

import jax
import jax.numpy as jnp
from jax import lax
from jax.experimental import pallas as pl
from jax.experimental.pallas import tpu as pltpu
from jax.sharding import PartitionSpec as P

MESH = pl.DeviceIdType.MESH
SPLIT = 4
EARLY = 3
FIRST = 128
SIDE = 4


def gather_kernel(
    banks, chips, w_hbm, avg_hbm, rw_hbm, gain_hbm,
    big, scale_ref, router_ref,
    wbuf, abuf, rw_ref, gain_ref, part, other, sums, total, rblk, from_l, from_r,
    wsem, asem, osem, ssem, tsem, tok_l, tok_r,
    rsem_r, rsem_l, send_r, send_l, esend_r, esend_l, erecv_r, erecv_l, send_p, recv_p, rsend, rrecv,
):
    experts, rows, lanes = wbuf.shape
    bank = lax.axis_index("bank")
    zero = lax.axis_index("zero")
    z = zero // 2
    core = zero % 2
    y, x = bank // SIDE, bank % SIDE
    tall = banks // SIDE
    right = {"zero": ((z + 1) % chips) * 2 + core}
    left = {"zero": ((z + chips - 1) % chips) * 2 + core}
    partner = {"zero": z * 2 + (1 - core)}
    x_up, x_down = {"bank": y * SIDE + (x + 1) % SIDE}, {"bank": y * SIDE + (x + SIDE - 1) % SIDE}
    y_up, y_down = {"bank": ((y + 1) % tall) * SIDE + x}, {"bank": ((y + tall - 1) % tall) * SIDE + x}
    half = experts // 2
    groups = rows // lanes
    piece = rows // SPLIT
    chunks = experts * SPLIT
    reach = chips // 2
    ahead = EARLY * piece

    def remote(src, dst, send, recv, to):
        return pltpu.make_async_remote_copy(src, dst, send, recv, device_id=to, device_id_type=MESH)

    def signal(sem, to):
        pl.semaphore_signal(sem, inc=1, device_id=to, device_id_type=MESH)

    small = [pltpu.make_async_copy(rw_hbm, rw_ref, asem.at[experts]),
             pltpu.make_async_copy(gain_hbm, gain_ref, wsem.at[experts])]
    loads = []
    for e in range(experts):
        lw = pltpu.make_async_copy(w_hbm.at[e], wbuf.at[e], wsem.at[e])
        la = pltpu.make_async_copy(avg_hbm.at[e], abuf.at[e], asem.at[e])
        lw.start()
        la.start()
        loads.append((lw, la))
    for copy in small:
        copy.start()

    barrier = pltpu.get_barrier_semaphore()
    near = (left, right, partner, x_up, x_down, y_up, y_down)
    for to in near:
        signal(barrier, to)

    eye = (
        lax.broadcasted_iota(jnp.int32, (lanes, lanes), 0)
        == lax.broadcasted_iota(jnp.int32, (lanes, lanes), 1)
    )

    def square(e):
        loads[e][0].wait()
        loads[e][1].wait()
        for g in range(groups):
            at = pl.ds(g * lanes, lanes)
            fresh = wbuf[e, at, :] + abuf[e, at, :].astype(jnp.float32)
            wbuf[e, at, :] = fresh
            row = jnp.sum(fresh * fresh, axis=1, keepdims=True)
            part[e, g:g + 1, :] = jnp.sum(jnp.where(eye, row, 0.0), axis=0, keepdims=True)

    def early(at):
        remote(wbuf.at[0, at], from_l.at[at], esend_r, erecv_r, right).start()
        remote(wbuf.at[0, at], from_r.at[at], esend_l, erecv_l, left).start()

    for e in range(half):
        square(e)
    pl.semaphore_wait(barrier, len(near))
    signal(tok_l.at[0], right)
    signal(tok_r.at[0], left)
    early(pl.ds(0, FIRST))
    for e in range(half, experts):
        square(e)

    mine, theirs = pl.ds(core * half, half), pl.ds((1 - core) * half, half)
    swap = remote(part.at[theirs], other, osem.at[0], osem.at[1], partner)
    swap.start()
    for d in range(2, reach + 1):
        pl.semaphore_wait(tok_l.at[d - 2], 1)
        if d < reach:
            signal(tok_l.at[d - 1], right)
            pl.semaphore_wait(tok_r.at[d - 2], 1)
            if d < reach - 1:
                signal(tok_r.at[d - 1], left)
    swap.wait_recv()
    sums[z] = part[mine] + other[...]
    peers = [{"zero": ((z + j) % chips) * 2 + core} for j in range(1, chips)]
    peers = sorted(zip(range(1, chips), peers), key=lambda p: -min(p[0], chips - p[0]))
    for _, to in peers:
        remote(sums.at[z], sums.at[z], ssem.at[0], ssem.at[1], to).start()
    if ahead > FIRST:
        for g in range(FIRST // lanes, ahead // lanes):
            early(pl.ds(g * lanes, lanes))
    for copy in small:
        copy.wait()
    rblk[core, bank, z] = rw_ref[...] * gain_ref[...]

    most = sums.at[pl.ds(0, chips - 1)]
    full = remote(most, most, ssem.at[0], ssem.at[1], partner)
    full.wait_recv()
    acc = sums[0]
    for k in range(1, chips):
        acc = acc + sums[k]
    total[mine] = acc
    back = remote(total.at[mine], total.at[mine], tsem.at[0], tsem.at[1], partner)
    back.start()
    back.wait_recv()

    def place(k, src):
        return big.at[k // SPLIT, pl.ds((k % SPLIT) * piece, piece),
                      pl.ds(pl.multiple_of(src * lanes, lanes), lanes)]

    def to_right(slot, k, src):
        return remote(place(k, src), place(k, src), send_r, rsem_r.at[slot], right)

    def to_left(slot, k, src):
        return remote(place(k, src), place(k, src), send_l, rsem_l.at[slot], left)

    def to_partner(k, src):
        return remote(place(k, src), place(k, src), send_p, recv_p, partner)

    def serve(k, src, read):
        e, s = k // SPLIT, k % SPLIT
        root = jnp.sqrt(total[e])
        columns = pl.ds(pl.multiple_of(src * lanes, lanes), lanes)
        for g in range(s * groups // SPLIT, (s + 1) * groups // SPLIT):
            at = pl.ds(g * lanes, lanes)
            col = jnp.sum(jnp.where(eye, root[g:g + 1, :], 0.0), axis=1, keepdims=True)
            big[e, at, columns] = (read(e, at) / col).astype(jnp.bfloat16)

    for k in [*range(EARLY, chunks), *range(EARLY)]:
        serve(k, zero, lambda e, at: wbuf[e, at, :])
        if k >= EARLY:
            to_right(k, k, zero).start()
            to_left(k, k, zero).start()
        to_partner(k, zero).start()
    for e in range(experts):
        root = jnp.sqrt(total[e])
        for g in range(groups):
            scale_ref[e:e + 1, g * lanes:(g + 1) * lanes] = root[g:g + 1, :]

    from_left = [{}] + [((z + chips - d) % chips) * 2 + core for d in range(1, reach + 1)]
    from_right = [{}] + [((z + d) % chips) * 2 + core for d in range(1, reach + 1)]

    def on_right(d, slot, k):
        if d < reach - 1:
            to_right(slot + chunks, k, from_left[d]).start()
        elif d == reach - 1 and k % 2 == 0:
            to_right(d * chunks + k // 2, k, from_left[d]).start()
        to_partner(k, from_left[d]).start()

    def on_left(d, slot, k):
        if d < reach - 1:
            to_left(slot + chunks, k, from_right[d]).start()
        elif d == reach - 1 and k % 2 == 1:
            to_left(d * chunks + k // 2, k, from_right[d]).start()
        to_partner(k, from_right[d]).start()

    rows_ahead = wbuf.at[0, pl.ds(0, ahead)]
    remote(rows_ahead, from_l, esend_r, erecv_r, right).wait_recv()
    remote(rows_ahead, from_r, esend_l, erecv_l, left).wait_recv()
    for k in range(EARLY):
        serve(k, from_left[1], lambda e, at: from_l[at, :])
        on_right(1, k, k)
        serve(k, from_right[1], lambda e, at: from_r[at, :])
        on_left(1, k, k)

    def router_z():
        for _, to in peers:
            remote(rblk.at[core, bank, z], rblk.at[core, bank, z], rsend.at[0], rrecv.at[0], to).start()

    def router_wait(n, ref):
        remote(ref, ref, rsend.at[n], rrecv.at[n], partner).wait()

    def router_x():
        router_wait(0, rblk.at[core, bank, pl.ds(0, chips - 1)])
        own = rblk.at[core, bank]
        remote(own, own, rsend.at[1], rrecv.at[1], x_up).start()
        remote(own, own, rsend.at[1], rrecv.at[1], x_down).start()

    def router_x2():
        router_wait(1, rblk.at[core, pl.ds(0, 2)])
        for j in range(2, SIDE - 1):
            own = rblk.at[core, y * SIDE + (x + SIDE + 1 - j) % SIDE]
            remote(own, own, rsend.at[2], rrecv.at[2], x_up).start()

    def router_y():
        router_wait(2, rblk.at[core, 0])
        own = rblk.at[core, pl.ds(y * SIDE, SIDE)]
        remote(own, own, rsend.at[3], rrecv.at[3], y_up).start()
        remote(own, own, rsend.at[3], rrecv.at[3], y_down).start()

    def router_y2():
        router_wait(3, rblk.at[core, pl.ds(0, 2 * SIDE)])
        own = rblk.at[core, pl.ds(((y + tall - 1) % tall) * SIDE, SIDE)]
        remote(own, own, rsend.at[4], rrecv.at[4], y_up).start()

    def router_partner():
        router_wait(4, rblk.at[core, pl.ds(0, SIDE)])
        remote(rblk.at[core], rblk.at[core], rsend.at[5], rrecv.at[5], partner).start()

    def router_finish():
        router_wait(5, rblk.at[core])
        for b in range(banks // 4):
            for q in range(2 * chips):
                block = jnp.concatenate([rblk[q % 2, 4 * b + i, q // 2] for i in range(4)], axis=0)
                n = block.shape[0]
                router_ref[b * n:(b + 1) * n, q * lanes:(q + 1) * lanes] = block.astype(jnp.bfloat16)

    router_steps = [router_x, router_x2, router_y, router_y2, router_partner, router_finish]
    router_z()

    slot = 0
    for d in range(1, reach + 1):
        last = d == reach
        for i in range(chunks // 2 if last else chunks):
            kr = 2 * i if last else i
            kl = 2 * i + 1 if last else i
            if d > 1 or i >= EARLY:
                to_right(slot, kr, from_left[d]).wait_recv()
                on_right(d, slot, kr)
                to_left(slot, kl, from_right[d]).wait_recv()
                on_left(d, slot, kl)
            slot += 1
            if slot % 8 == 0 and router_steps:
                router_steps.pop(0)()

    full.wait_send()
    swap.wait_send()
    back.wait_send()
    remote(rows_ahead, from_l, esend_r, erecv_r, right).wait_send()
    remote(rows_ahead, from_r, esend_l, erecv_l, left).wait_send()
    sent = (chunks * (chips - 1) // 2 - EARLY) * piece // (2 * chips)
    hops = big.at[0, pl.ds(0, sent), :]
    remote(hops, hops, send_r, rsem_r.at[0], right).wait_send()
    remote(hops, hops, send_l, rsem_l.at[0], left).wait_send()
    whole = big.at[:, :, pl.ds(0, chips * lanes)]
    remote(whole, whole, send_p, recv_p, partner).wait()


def out_kernel(big, scale, router, big_hbm, scale_hbm, router_hbm, sems):
    n = big.shape[0]
    copies = [pltpu.make_async_copy(big.at[e], big_hbm.at[e], sems.at[e]) for e in range(n)]
    copies.append(pltpu.make_async_copy(scale, scale_hbm, sems.at[n]))
    copies.append(pltpu.make_async_copy(router, router_hbm, sems.at[n + 1]))
    for copy in copies:
        copy.start()
    for copy in copies:
        copy.wait()


def solution(mesh):
    banks, zeros = mesh.shape["bank"], mesh.shape["zero"]
    chips = zeros // 2

    def shards(w_down, avg_down, router_weight, router_gain):
        experts, rows, lanes = w_down.shape
        width = lanes * zeros
        cols = router_weight.shape[1]
        vmem = pl.BlockSpec(memory_space=pltpu.VMEM)
        hbm = pl.BlockSpec(memory_space=pltpu.HBM)
        pin = lambda x: pltpu.with_memory_space_constraint(x, pltpu.HBM)
        half = experts // 2
        groups = rows // lanes
        slots = experts * SPLIT * (chips - 1) // 2
        ahead = EARLY * rows // SPLIT
        reach = chips // 2
        dma = pltpu.SemaphoreType.DMA
        regular = pltpu.SemaphoreType.REGULAR
        big, scale, router = pl.pallas_call(
            functools.partial(gather_kernel, banks, chips),
            out_shape=(
                jax.ShapeDtypeStruct((experts, rows, width), jnp.bfloat16),
                jax.ShapeDtypeStruct((experts, rows), jnp.float32),
                jax.ShapeDtypeStruct((cols * banks, width), jnp.bfloat16),
            ),
            in_specs=[hbm] * 4,
            out_specs=(vmem, vmem, vmem),
            scratch_shapes=[
                pltpu.VMEM((experts, rows, lanes), jnp.float32),
                pltpu.VMEM((experts, rows, lanes), jnp.bfloat16),
                pltpu.VMEM((cols, lanes), jnp.float32),
                pltpu.VMEM((1, lanes), jnp.float32),
                pltpu.VMEM((experts, groups, lanes), jnp.float32),
                pltpu.VMEM((half, groups, lanes), jnp.float32),
                pltpu.VMEM((chips, half, groups, lanes), jnp.float32),
                pltpu.VMEM((experts, groups, lanes), jnp.float32),
                pltpu.VMEM((2, banks, chips, cols, lanes), jnp.float32),
                pltpu.VMEM((ahead, lanes), jnp.float32),
                pltpu.VMEM((ahead, lanes), jnp.float32),
                dma((experts + 1,)), dma((experts + 1,)), dma((2,)), dma((2,)), dma((2,)),
                regular((reach - 1,)), regular((reach - 2,)),
                dma((slots,)), dma((slots,)), dma(()), dma(()), dma(()), dma(()), dma(()), dma(()),
                dma(()), dma(()), dma((6,)), dma((6,)),
            ],
            compiler_params=pltpu.CompilerParams(
                collective_id=0, has_side_effects=True, vmem_limit_bytes=8 * 1024 * 1024),
            name="gather",
        )(pin(w_down), pin(avg_down), pin(router_weight.T), pin(router_gain.reshape(1, lanes)))
        big, scale, router = pl.pallas_call(
            out_kernel,
            out_shape=(
                jax.ShapeDtypeStruct(big.shape, big.dtype),
                jax.ShapeDtypeStruct(scale.shape, scale.dtype),
                jax.ShapeDtypeStruct(router.shape, router.dtype),
            ),
            in_specs=[vmem, vmem, vmem],
            out_specs=(hbm, hbm, hbm),
            scratch_shapes=[dma((experts + 2,))],
            compiler_params=pltpu.CompilerParams(vmem_limit_bytes=4 * 1024 * 1024),
            name="put_out",
        )(big, scale, router)
        return big, scale, router.T

    return jax.shard_map(
        shards,
        mesh=mesh,
        in_specs=(P("bank", None, "zero"), P("bank", None, "zero"), P("zero", "bank"), P("zero")),
        out_specs=(P("bank", None, None), P("bank", None), P()),
        check_vma=False,
    )
```

```python
import functools

import jax
import jax.numpy as jnp
from jax import lax
from jax.experimental import pallas as pl
from jax.experimental.pallas import tpu as pltpu
from jax.sharding import PartitionSpec as P

MESH = pl.DeviceIdType.MESH
SPLIT = 2
EARLY = (2, 0)
SIDE = 4


def gather_kernel(
    banks, chips, w_hbm, avg_hbm, rw_hbm, gain_hbm,
    big, scale_ref, router_ref,
    wbuf, abuf, rw_ref, gain_ref, part, other, sums, total, rblk, from_l, from_r,
    wsem, asem, osem, ssem, tsem, tok_l, tok_r,
    rsem_r, rsem_l, send_r, send_l, esend_r, esend_l, erecv_r, erecv_l, send_p, recv_p, rsend, rrecv,
):
    experts, rows, lanes = wbuf.shape
    bank = lax.axis_index("bank")
    zero = lax.axis_index("zero")
    z = zero // 2
    core = zero % 2
    y, x = bank // SIDE, bank % SIDE
    tall = banks // SIDE
    right = {"zero": ((z + 1) % chips) * 2 + core}
    left = {"zero": ((z + chips - 1) % chips) * 2 + core}
    partner = {"zero": z * 2 + (1 - core)}
    x_up, x_down = {"bank": y * SIDE + (x + 1) % SIDE}, {"bank": y * SIDE + (x + SIDE - 1) % SIDE}
    y_up, y_down = {"bank": ((y + 1) % tall) * SIDE + x}, {"bank": ((y + tall - 1) % tall) * SIDE + x}
    groups = rows // lanes
    piece = rows // SPLIT
    chunks = experts * SPLIT
    reach = chips // 2
    early = EARLY[1] + (EARLY[0] - EARLY[1]) * (1 - core)

    def remote(src, dst, send, recv, to):
        return pltpu.make_async_remote_copy(src, dst, send, recv, device_id=to, device_id_type=MESH)

    def signal(sem, to):
        pl.semaphore_signal(sem, inc=1, device_id=to, device_id_type=MESH)

    small = [pltpu.make_async_copy(rw_hbm, rw_ref, asem.at[experts]),
             pltpu.make_async_copy(gain_hbm, gain_ref, wsem.at[experts])]
    loads = []
    for e in range(experts):
        lw = pltpu.make_async_copy(w_hbm.at[e], wbuf.at[e], wsem.at[e])
        la = pltpu.make_async_copy(avg_hbm.at[e], abuf.at[e], asem.at[e])
        lw.start()
        la.start()
        loads.append((lw, la))
    for copy in small:
        copy.start()

    barrier = pltpu.get_barrier_semaphore()
    near = (left, right, partner, x_up, x_down, y_up, y_down)
    for to in near:
        signal(barrier, to)

    eye = (
        lax.broadcasted_iota(jnp.int32, (lanes, lanes), 0)
        == lax.broadcasted_iota(jnp.int32, (lanes, lanes), 1)
    )

    def square(e):
        loads[e][0].wait()
        loads[e][1].wait()
        for g in range(groups):
            at = pl.ds(g * lanes, lanes)
            fresh = wbuf[e, at, :] + abuf[e, at, :].astype(jnp.float32)
            wbuf[e, at, :] = fresh
            row = jnp.sum(fresh * fresh, axis=1, keepdims=True)
            part[e, g:g + 1, :] = jnp.sum(jnp.where(eye, row, 0.0), axis=0, keepdims=True)

    def ahead(k):
        return wbuf.at[k // SPLIT, pl.ds(pl.multiple_of(k % SPLIT * piece, piece), piece)]

    def early_right(k):
        return remote(ahead(k), from_l.at[k], esend_r, erecv_r.at[k], right)

    def early_left(k):
        return remote(ahead(k), from_r.at[k], esend_l, erecv_l.at[k], left)

    def send_early(k, _):
        early_right(k).start()
        early_left(k).start()
        return 0

    first, second = core == 0, core == 1

    square(0)
    pl.semaphore_wait(barrier, len(near))
    signal(tok_l.at[0], right)
    signal(tok_r.at[0], left)
    for e in range(1, experts + 1):
        if e * SPLIT - SPLIT < EARLY[0]:
            @pl.when(first)
            def _():
                lax.fori_loop(e * SPLIT - SPLIT, min(e * SPLIT, EARLY[0]), send_early, 0)
        if e < experts:
            square(e)

    swap = remote(part, other, osem.at[0], osem.at[1], partner)
    back = remote(total, total, tsem.at[0], tsem.at[1], partner)
    peers = [{"zero": ((z + j) % chips) * 2 + core} for j in range(1, chips)]
    peers = [to for _, to in sorted(zip(range(1, chips), peers), key=lambda p: -min(p[0], chips - p[0]))]
    most = sums.at[pl.ds(0, chips - 1)]
    full = remote(most, most, ssem.at[0], ssem.at[1], partner)

    @pl.when(first)
    def _():
        swap.start()

    for d in range(2, reach + 1):
        pl.semaphore_wait(tok_l.at[d - 2], 1)
        if d < reach:
            signal(tok_l.at[d - 1], right)
            pl.semaphore_wait(tok_r.at[d - 2], 1)
            if d < reach - 1:
                signal(tok_r.at[d - 1], left)

    @pl.when(second)
    def _():
        swap.wait_recv()
        sums[z] = part[...] + other[...]
        for to in peers:
            remote(sums.at[z], sums.at[z], ssem.at[0], ssem.at[1], to).start()
        lax.fori_loop(0, EARLY[1], send_early, 0)

    for copy in small:
        copy.wait()
    rblk[core, bank, z] = rw_ref[...] * gain_ref[...]

    @pl.when(second)
    def _():
        full.wait_recv()
        acc = sums[0]
        for k in range(1, chips):
            acc = acc + sums[k]
        total[...] = acc
        back.start()

    @pl.when(first)
    def _():
        back.wait_recv()

    def place(k, src):
        return big.at[k // SPLIT, pl.ds(pl.multiple_of(k % SPLIT * piece, piece), piece),
                      pl.ds(pl.multiple_of(src * lanes, lanes), lanes)]

    def to_right(slot, k, src):
        return remote(place(k, src), place(k, src), send_r, rsem_r.at[slot], right)

    def to_left(slot, k, src):
        return remote(place(k, src), place(k, src), send_l, rsem_l.at[slot], left)

    def to_partner(k, src):
        return remote(place(k, src), place(k, src), send_p, recv_p, partner)

    def serve(k, src, read):
        e = k // SPLIT
        columns = pl.ds(pl.multiple_of(src * lanes, lanes), lanes)
        for j in range(groups // SPLIT):
            g = k % SPLIT * (groups // SPLIT) + j
            at = pl.ds(pl.multiple_of(g * lanes, lanes), lanes)
            root = jnp.sqrt(total[e, pl.ds(g, 1), :])
            col = jnp.sum(jnp.where(eye, root, 0.0), axis=1, keepdims=True)
            big[e, at, columns] = (read(j) / col).astype(jnp.bfloat16)

    def own(k):
        def read(j):
            g = k % SPLIT * (groups // SPLIT) + j
            return wbuf[k // SPLIT, pl.ds(pl.multiple_of(g * lanes, lanes), lanes), :]
        serve(k, zero, read)
        to_partner(k, zero).start()

    def own_late(k, _):
        own(k)
        to_right(k, k, zero).start()
        to_left(k, k, zero).start()
        return 0

    def own_early(k, _):
        own(k)
        return 0

    lax.fori_loop(early, chunks, own_late, 0)
    lax.fori_loop(0, early, own_early, 0)
    for e in range(experts):
        root = jnp.sqrt(total[e])
        for g in range(groups):
            scale_ref[e:e + 1, g * lanes:(g + 1) * lanes] = root[g:g + 1, :]

    from_left = [{}] + [((z + chips - d) % chips) * 2 + core for d in range(1, reach + 1)]
    from_right = [{}] + [((z + d) % chips) * 2 + core for d in range(1, reach + 1)]

    def on_right(d, slot, k):
        if d < reach - 1:
            to_right(slot + chunks, k, from_left[d]).start()
        elif d == reach - 1 and k % 2 == 0:
            to_right(d * chunks + k // 2, k, from_left[d]).start()
        to_partner(k, from_left[d]).start()

    def on_left(d, slot, k):
        if d < reach - 1:
            to_left(slot + chunks, k, from_right[d]).start()
        elif d == reach - 1 and k % 2 == 1:
            to_left(d * chunks + k // 2, k, from_right[d]).start()
        to_partner(k, from_right[d]).start()

    def convert(k, _):
        early_right(k).wait_recv()
        serve(k, from_left[1], lambda j: from_l[k, j * lanes:(j + 1) * lanes, :])
        on_right(1, k, k)
        early_left(k).wait_recv()
        serve(k, from_right[1], lambda j: from_r[k, j * lanes:(j + 1) * lanes, :])
        on_left(1, k, k)
        return 0

    def pass_on(k, _):
        to_right(k, k, from_left[1]).wait_recv()
        on_right(1, k, k)
        to_left(k, k, from_right[1]).wait_recv()
        on_left(1, k, k)
        return 0

    def router_z():
        for to in peers:
            remote(rblk.at[core, bank, z], rblk.at[core, bank, z], rsend.at[0], rrecv.at[0], to).start()

    def router_wait(n, ref):
        remote(ref, ref, rsend.at[n], rrecv.at[n], partner).wait()

    def router_x():
        router_wait(0, rblk.at[core, bank, pl.ds(0, chips - 1)])
        own = rblk.at[core, bank]
        remote(own, own, rsend.at[1], rrecv.at[1], x_up).start()
        remote(own, own, rsend.at[1], rrecv.at[1], x_down).start()

    def router_x2():
        router_wait(1, rblk.at[core, pl.ds(0, 2)])
        for j in range(2, SIDE - 1):
            own = rblk.at[core, y * SIDE + (x + SIDE + 1 - j) % SIDE]
            remote(own, own, rsend.at[2], rrecv.at[2], x_up).start()

    def router_y():
        router_wait(2, rblk.at[core, 0])
        own = rblk.at[core, pl.ds(y * SIDE, SIDE)]
        remote(own, own, rsend.at[3], rrecv.at[3], y_up).start()
        remote(own, own, rsend.at[3], rrecv.at[3], y_down).start()

    def router_y2():
        router_wait(3, rblk.at[core, pl.ds(0, 2 * SIDE)])
        own = rblk.at[core, pl.ds(((y + tall - 1) % tall) * SIDE, SIDE)]
        remote(own, own, rsend.at[4], rrecv.at[4], y_up).start()

    def router_partner():
        router_wait(4, rblk.at[core, pl.ds(0, SIDE)])
        remote(rblk.at[core], rblk.at[core], rsend.at[5], rrecv.at[5], partner).start()

    def router_finish():
        router_wait(5, rblk.at[core])
        for b in range(banks // 4):
            for q in range(2 * chips):
                block = jnp.concatenate([rblk[q % 2, 4 * b + i, q // 2] for i in range(4)], axis=0)
                n = block.shape[0]
                router_ref[b * n:(b + 1) * n, q * lanes:(q + 1) * lanes] = block.astype(jnp.bfloat16)

    router_steps = [router_x, router_x2, router_y, router_y2, router_partner, router_finish]
    router_z()

    lax.fori_loop(0, early, convert, 0)
    lax.fori_loop(early, chunks, pass_on, 0)
    router_steps.pop(0)()
    slot = chunks
    for d in range(2, reach + 1):
        last = d == reach
        for i in range(chunks // 2 if last else chunks):
            kr = 2 * i if last else i
            kl = 2 * i + 1 if last else i
            to_right(slot, kr, from_left[d]).wait_recv()
            on_right(d, slot, kr)
            to_left(slot, kl, from_right[d]).wait_recv()
            on_left(d, slot, kl)
            slot += 1
            if slot % 4 == 2 and router_steps:
                router_steps.pop(0)()

    for side in range(2):
        @pl.when(core == side)
        def _():
            if side == 0:
                swap.wait_send()
            else:
                full.wait_send()
                back.wait_send()
            if EARLY[side] > 0:
                rows_ahead = from_l.at[pl.ds(0, EARLY[side])]
                remote(rows_ahead, rows_ahead, esend_r, erecv_r.at[0], right).wait_send()
                remote(rows_ahead, rows_ahead, esend_l, erecv_l.at[0], left).wait_send()
            sent = (chunks * (chips - 1) // 2 - EARLY[side]) * piece // (2 * chips)
            hops = big.at[0, pl.ds(0, sent), :]
            remote(hops, hops, send_r, rsem_r.at[0], right).wait_send()
            remote(hops, hops, send_l, rsem_l.at[0], left).wait_send()
    whole = big.at[:, :, pl.ds(0, chips * lanes)]
    remote(whole, whole, send_p, recv_p, partner).wait()


def out_kernel(big, scale, router, big_hbm, scale_hbm, router_hbm, sems):
    n = big.shape[0]
    copies = [pltpu.make_async_copy(big.at[e], big_hbm.at[e], sems.at[e]) for e in range(n)]
    copies.append(pltpu.make_async_copy(scale, scale_hbm, sems.at[n]))
    copies.append(pltpu.make_async_copy(router, router_hbm, sems.at[n + 1]))
    for copy in copies:
        copy.start()
    for copy in copies:
        copy.wait()


def solution(mesh):
    banks, zeros = mesh.shape["bank"], mesh.shape["zero"]
    chips = zeros // 2

    def shards(w_down, avg_down, router_weight, router_gain):
        experts, rows, lanes = w_down.shape
        width = lanes * zeros
        cols = router_weight.shape[1]
        vmem = pl.BlockSpec(memory_space=pltpu.VMEM)
        hbm = pl.BlockSpec(memory_space=pltpu.HBM)
        pin = lambda x: pltpu.with_memory_space_constraint(x, pltpu.HBM)
        groups = rows // lanes
        slots = experts * SPLIT * (chips - 1) // 2
        chunk = (max(*EARLY, 1), rows // SPLIT, lanes)
        reach = chips // 2
        dma = pltpu.SemaphoreType.DMA
        regular = pltpu.SemaphoreType.REGULAR
        big, scale, router = pl.pallas_call(
            functools.partial(gather_kernel, banks, chips),
            out_shape=(
                jax.ShapeDtypeStruct((experts, rows, width), jnp.bfloat16),
                jax.ShapeDtypeStruct((experts, rows), jnp.float32),
                jax.ShapeDtypeStruct((cols * banks, width), jnp.bfloat16),
            ),
            in_specs=[hbm] * 4,
            out_specs=(vmem, vmem, vmem),
            scratch_shapes=[
                pltpu.VMEM((experts, rows, lanes), jnp.float32),
                pltpu.VMEM((experts, rows, lanes), jnp.bfloat16),
                pltpu.VMEM((cols, lanes), jnp.float32),
                pltpu.VMEM((1, lanes), jnp.float32),
                pltpu.VMEM((experts, groups, lanes), jnp.float32),
                pltpu.VMEM((experts, groups, lanes), jnp.float32),
                pltpu.VMEM((chips, experts, groups, lanes), jnp.float32),
                pltpu.VMEM((experts, groups, lanes), jnp.float32),
                pltpu.VMEM((2, banks, chips, cols, lanes), jnp.float32),
                pltpu.VMEM(chunk, jnp.float32),
                pltpu.VMEM(chunk, jnp.float32),
                dma((experts + 1,)), dma((experts + 1,)), dma((2,)), dma((2,)), dma((2,)),
                regular((reach - 1,)), regular((reach - 2,)),
                dma((slots,)), dma((slots,)), dma(()), dma(()), dma(()), dma(()), dma(chunk[:1]), dma(chunk[:1]),
                dma(()), dma(()), dma((6,)), dma((6,)),
            ],
            compiler_params=pltpu.CompilerParams(
                collective_id=0, has_side_effects=True, vmem_limit_bytes=12 * 1024 * 1024),
            name="gather",
        )(pin(w_down), pin(avg_down), pin(router_weight.T), pin(router_gain.reshape(1, lanes)))
        big, scale, router = pl.pallas_call(
            out_kernel,
            out_shape=(
                jax.ShapeDtypeStruct(big.shape, big.dtype),
                jax.ShapeDtypeStruct(scale.shape, scale.dtype),
                jax.ShapeDtypeStruct(router.shape, router.dtype),
            ),
            in_specs=[vmem, vmem, vmem],
            out_specs=(hbm, hbm, hbm),
            scratch_shapes=[dma((experts + 2,))],
            compiler_params=pltpu.CompilerParams(vmem_limit_bytes=4 * 1024 * 1024),
            name="put_out",
        )(big, scale, router)
        return big, scale, router.T

    return jax.shard_map(
        shards,
        mesh=mesh,
        in_specs=(P("bank", None, "zero"), P("bank", None, "zero"), P("zero", "bank"), P("zero")),
        out_specs=(P("bank", None, None), P("bank", None), P()),
        check_vma=False,
    )
```

```python
import functools

import jax
import jax.numpy as jnp
from jax import lax
from jax.experimental import pallas as pl
from jax.experimental.pallas import tpu as pltpu
from jax.sharding import PartitionSpec as P

MESH = pl.DeviceIdType.MESH
SPLIT = 2
EARLY = (2, 0)
SIDE = 4
PLANE = 1


def gather_kernel(
    banks, chips, w_hbm, avg_hbm, rw_hbm, gain_hbm,
    big, scale_ref, router_ref,
    wbuf, abuf, rw_ref, gain_ref, part, other, sums, total, rblk, from_l, from_r,
    wsem, asem, osem, ssem, tsem, tok_l, tok_r, tok_x, tok_z,
    rsem_r, rsem_l, send_r, send_l, esend_r, esend_l, erecv_r, erecv_l, send_p, recv_p, rsend, rrecv,
):
    experts, rows, lanes = wbuf.shape
    bank = lax.axis_index("bank")
    zero = lax.axis_index("zero")
    z = zero // 2
    core = zero % 2
    y, x = bank // SIDE, bank % SIDE
    tall = banks // SIDE
    right = {"zero": ((z + 1) % chips) * 2 + core}
    left = {"zero": ((z + chips - 1) % chips) * 2 + core}
    partner = {"zero": z * 2 + (1 - core)}
    x_up, x_down = {"bank": y * SIDE + (x + 1) % SIDE}, {"bank": y * SIDE + (x + SIDE - 1) % SIDE}
    y_up, y_down = {"bank": ((y + 1) % tall) * SIDE + x}, {"bank": ((y + tall - 1) % tall) * SIDE + x}
    groups = rows // lanes
    piece = rows // SPLIT
    chunks = experts * SPLIT
    reach = chips // 2
    early = EARLY[1] + (EARLY[0] - EARLY[1]) * (1 - core)

    def remote(src, dst, send, recv, to):
        return pltpu.make_async_remote_copy(src, dst, send, recv, device_id=to, device_id_type=MESH)

    def signal(sem, to):
        pl.semaphore_signal(sem, inc=1, device_id=to, device_id_type=MESH)

    small = [pltpu.make_async_copy(rw_hbm, rw_ref, asem.at[experts]),
             pltpu.make_async_copy(gain_hbm, gain_ref, wsem.at[experts])]
    loads = []
    for e in range(experts):
        lw = pltpu.make_async_copy(w_hbm.at[e], wbuf.at[e], wsem.at[e])
        la = pltpu.make_async_copy(avg_hbm.at[e], abuf.at[e], asem.at[e])
        lw.start()
        la.start()
        loads.append((lw, la))
    for copy in small:
        copy.start()

    barrier = pltpu.get_barrier_semaphore()
    near, across = (left, right, partner), (x_up, x_down, y_up, y_down)
    for to in near:
        signal(barrier, to)

    @pl.when(z == PLANE)
    def _():
        for to in across:
            signal(barrier, to)

    eye = (
        lax.broadcasted_iota(jnp.int32, (lanes, lanes), 0)
        == lax.broadcasted_iota(jnp.int32, (lanes, lanes), 1)
    )

    def square(e):
        loads[e][0].wait()
        loads[e][1].wait()
        for g in range(groups):
            at = pl.ds(g * lanes, lanes)
            fresh = wbuf[e, at, :] + abuf[e, at, :].astype(jnp.float32)
            wbuf[e, at, :] = fresh
            row = jnp.sum(fresh * fresh, axis=1, keepdims=True)
            part[e, g:g + 1, :] = jnp.sum(jnp.where(eye, row, 0.0), axis=0, keepdims=True)

    def ahead(k):
        return wbuf.at[k // SPLIT, pl.ds(pl.multiple_of(k % SPLIT * piece, piece), piece)]

    def early_right(k):
        return remote(ahead(k), from_l.at[k], esend_r, erecv_r.at[k], right)

    def early_left(k):
        return remote(ahead(k), from_r.at[k], esend_l, erecv_l.at[k], left)

    def send_early(k, _):
        early_right(k).start()
        early_left(k).start()
        return 0

    first, second = core == 0, core == 1

    square(0)
    @pl.when(z == PLANE)
    def _():
        pl.semaphore_wait(barrier, len(near) + len(across))

    @pl.when(z != PLANE)
    def _():
        pl.semaphore_wait(barrier, len(near))

    signal(tok_l.at[0], right)
    signal(tok_r.at[0], left)
    for e in range(1, experts + 1):
        if e * SPLIT - SPLIT < EARLY[0]:
            @pl.when(first)
            def _():
                lax.fori_loop(e * SPLIT - SPLIT, min(e * SPLIT, EARLY[0]), send_early, 0)
        if e < experts:
            square(e)

    swap = remote(part, other, osem.at[0], osem.at[1], partner)
    back = remote(total, total, tsem.at[0], tsem.at[1], partner)
    peers = [{"zero": ((z + j) % chips) * 2 + core} for j in range(1, chips)]
    peers = [to for _, to in sorted(zip(range(1, chips), peers), key=lambda p: -min(p[0], chips - p[0]))]
    most = sums.at[pl.ds(0, chips - 1)]
    full = remote(most, most, ssem.at[0], ssem.at[1], partner)

    @pl.when(first)
    def _():
        swap.start()

    for d in range(2, reach + 1):
        pl.semaphore_wait(tok_l.at[d - 2], 1)
        if d < reach:
            signal(tok_l.at[d - 1], right)
            pl.semaphore_wait(tok_r.at[d - 2], 1)
            if d < reach - 1:
                signal(tok_r.at[d - 1], left)

    @pl.when(second)
    def _():
        swap.wait_recv()
        sums[z] = part[...] + other[...]
        for to in peers:
            remote(sums.at[z], sums.at[z], ssem.at[0], ssem.at[1], to).start()
        lax.fori_loop(0, EARLY[1], send_early, 0)

    @pl.when(z == PLANE)
    def _():
        for to in across:
            signal(tok_x, to)

    for copy in small:
        copy.wait()
    rblk[core, bank, z] = rw_ref[...] * gain_ref[...]

    @pl.when(second)
    def _():
        full.wait_recv()
        acc = sums[0]
        for k in range(1, chips):
            acc = acc + sums[k]
        total[...] = acc
        back.start()

    @pl.when(first)
    def _():
        back.wait_recv()

    def place(k, src):
        return big.at[k // SPLIT, pl.ds(pl.multiple_of(k % SPLIT * piece, piece), piece),
                      pl.ds(pl.multiple_of(src * lanes, lanes), lanes)]

    def to_right(slot, k, src):
        return remote(place(k, src), place(k, src), send_r, rsem_r.at[slot], right)

    def to_left(slot, k, src):
        return remote(place(k, src), place(k, src), send_l, rsem_l.at[slot], left)

    def to_partner(k, src):
        return remote(place(k, src), place(k, src), send_p, recv_p, partner)

    def serve(k, src, read):
        e = k // SPLIT
        columns = pl.ds(pl.multiple_of(src * lanes, lanes), lanes)
        for j in range(groups // SPLIT):
            g = k % SPLIT * (groups // SPLIT) + j
            at = pl.ds(pl.multiple_of(g * lanes, lanes), lanes)
            root = jnp.sqrt(total[e, pl.ds(g, 1), :])
            col = jnp.sum(jnp.where(eye, root, 0.0), axis=1, keepdims=True)
            big[e, at, columns] = (read(j) / col).astype(jnp.bfloat16)

    def own(k):
        def read(j):
            g = k % SPLIT * (groups // SPLIT) + j
            return wbuf[k // SPLIT, pl.ds(pl.multiple_of(g * lanes, lanes), lanes), :]
        serve(k, zero, read)
        to_partner(k, zero).start()

    def own_late(k, _):
        own(k)
        to_right(k, k, zero).start()
        to_left(k, k, zero).start()
        return 0

    def own_early(k, _):
        own(k)
        return 0

    lax.fori_loop(early, chunks, own_late, 0)
    lax.fori_loop(0, early, own_early, 0)
    for e in range(experts):
        root = jnp.sqrt(total[e])
        for g in range(groups):
            scale_ref[e:e + 1, g * lanes:(g + 1) * lanes] = root[g:g + 1, :]

    from_left = [{}] + [((z + chips - d) % chips) * 2 + core for d in range(1, reach + 1)]
    from_right = [{}] + [((z + d) % chips) * 2 + core for d in range(1, reach + 1)]

    def on_right(d, slot, k):
        if d < reach - 1:
            to_right(slot + chunks, k, from_left[d]).start()
        elif d == reach - 1 and k % 2 == 0:
            to_right(d * chunks + k // 2, k, from_left[d]).start()
        to_partner(k, from_left[d]).start()

    def on_left(d, slot, k):
        if d < reach - 1:
            to_left(slot + chunks, k, from_right[d]).start()
        elif d == reach - 1 and k % 2 == 1:
            to_left(d * chunks + k // 2, k, from_right[d]).start()
        to_partner(k, from_right[d]).start()

    def convert(k, _):
        early_right(k).wait_recv()
        serve(k, from_left[1], lambda j: from_l[k, j * lanes:(j + 1) * lanes, :])
        on_right(1, k, k)
        early_left(k).wait_recv()
        serve(k, from_right[1], lambda j: from_r[k, j * lanes:(j + 1) * lanes, :])
        on_left(1, k, k)
        return 0

    def pass_on(k, _):
        to_right(k, k, from_left[1]).wait_recv()
        on_right(1, k, k)
        to_left(k, k, from_right[1]).wait_recv()
        on_left(1, k, k)
        return 0

    def router_z():
        for to in peers:
            remote(rblk.at[core, bank, z], rblk.at[core, bank, z], rsend.at[0], rrecv.at[0], to).start()

    def router_wait(n, ref):
        remote(ref, ref, rsend.at[n], rrecv.at[n], partner).wait()

    def router_x():
        router_wait(0, rblk.at[core, bank, pl.ds(0, chips - 1)])

        @pl.when(z == PLANE)
        def _():
            pl.semaphore_wait(tok_x, len(across))
            for to in peers:
                signal(tok_z, to)

        @pl.when(z != PLANE)
        def _():
            pl.semaphore_wait(tok_z, 1)

        own = rblk.at[core, bank]
        remote(own, own, rsend.at[1], rrecv.at[1], x_up).start()
        remote(own, own, rsend.at[1], rrecv.at[1], x_down).start()

    def router_x2():
        router_wait(1, rblk.at[core, pl.ds(0, 2)])
        for j in range(2, SIDE - 1):
            own = rblk.at[core, y * SIDE + (x + SIDE + 1 - j) % SIDE]
            remote(own, own, rsend.at[2], rrecv.at[2], x_up).start()

    def router_y():
        router_wait(2, rblk.at[core, 0])
        own = rblk.at[core, pl.ds(y * SIDE, SIDE)]
        remote(own, own, rsend.at[3], rrecv.at[3], y_up).start()
        remote(own, own, rsend.at[3], rrecv.at[3], y_down).start()

    def router_y2():
        router_wait(3, rblk.at[core, pl.ds(0, 2 * SIDE)])
        own = rblk.at[core, pl.ds(((y + tall - 1) % tall) * SIDE, SIDE)]
        remote(own, own, rsend.at[4], rrecv.at[4], y_up).start()

    def router_partner():
        router_wait(4, rblk.at[core, pl.ds(0, SIDE)])
        remote(rblk.at[core], rblk.at[core], rsend.at[5], rrecv.at[5], partner).start()

    def router_finish():
        router_wait(5, rblk.at[core])
        for b in range(banks // 4):
            for q in range(2 * chips):
                block = jnp.concatenate([rblk[q % 2, 4 * b + i, q // 2] for i in range(4)], axis=0)
                n = block.shape[0]
                router_ref[b * n:(b + 1) * n, q * lanes:(q + 1) * lanes] = block.astype(jnp.bfloat16)

    router_steps = [router_x, router_x2, router_y, router_y2, router_partner, router_finish]
    router_z()

    lax.fori_loop(0, early, convert, 0)
    lax.fori_loop(early, chunks, pass_on, 0)
    router_steps.pop(0)()
    slot = chunks
    for d in range(2, reach + 1):
        last = d == reach
        for i in range(chunks // 2 if last else chunks):
            kr = 2 * i if last else i
            kl = 2 * i + 1 if last else i
            to_right(slot, kr, from_left[d]).wait_recv()
            on_right(d, slot, kr)
            to_left(slot, kl, from_right[d]).wait_recv()
            on_left(d, slot, kl)
            slot += 1
            if slot % 4 == 2 and router_steps:
                router_steps.pop(0)()

    for side in range(2):
        @pl.when(core == side)
        def _():
            if side == 0:
                swap.wait_send()
            else:
                full.wait_send()
                back.wait_send()
            if EARLY[side] > 0:
                rows_ahead = from_l.at[pl.ds(0, EARLY[side])]
                remote(rows_ahead, rows_ahead, esend_r, erecv_r.at[0], right).wait_send()
                remote(rows_ahead, rows_ahead, esend_l, erecv_l.at[0], left).wait_send()
            sent = (chunks * (chips - 1) // 2 - EARLY[side]) * piece // (2 * chips)
            hops = big.at[0, pl.ds(0, sent), :]
            remote(hops, hops, send_r, rsem_r.at[0], right).wait_send()
            remote(hops, hops, send_l, rsem_l.at[0], left).wait_send()
    whole = big.at[:, :, pl.ds(0, chips * lanes)]
    remote(whole, whole, send_p, recv_p, partner).wait()


def out_kernel(big, scale, router, big_hbm, scale_hbm, router_hbm, sems):
    n = big.shape[0]
    copies = [pltpu.make_async_copy(big.at[e], big_hbm.at[e], sems.at[e]) for e in range(n)]
    copies.append(pltpu.make_async_copy(scale, scale_hbm, sems.at[n]))
    copies.append(pltpu.make_async_copy(router, router_hbm, sems.at[n + 1]))
    for copy in copies:
        copy.start()
    for copy in copies:
        copy.wait()


def solution(mesh):
    banks, zeros = mesh.shape["bank"], mesh.shape["zero"]
    chips = zeros // 2

    def shards(w_down, avg_down, router_weight, router_gain):
        experts, rows, lanes = w_down.shape
        width = lanes * zeros
        cols = router_weight.shape[1]
        vmem = pl.BlockSpec(memory_space=pltpu.VMEM)
        hbm = pl.BlockSpec(memory_space=pltpu.HBM)
        pin = lambda x: pltpu.with_memory_space_constraint(x, pltpu.HBM)
        groups = rows // lanes
        slots = experts * SPLIT * (chips - 1) // 2
        chunk = (max(*EARLY, 1), rows // SPLIT, lanes)
        reach = chips // 2
        dma = pltpu.SemaphoreType.DMA
        regular = pltpu.SemaphoreType.REGULAR
        big, scale, router = pl.pallas_call(
            functools.partial(gather_kernel, banks, chips),
            out_shape=(
                jax.ShapeDtypeStruct((experts, rows, width), jnp.bfloat16),
                jax.ShapeDtypeStruct((experts, rows), jnp.float32),
                jax.ShapeDtypeStruct((cols * banks, width), jnp.bfloat16),
            ),
            in_specs=[hbm] * 4,
            out_specs=(vmem, vmem, vmem),
            scratch_shapes=[
                pltpu.VMEM((experts, rows, lanes), jnp.float32),
                pltpu.VMEM((experts, rows, lanes), jnp.bfloat16),
                pltpu.VMEM((cols, lanes), jnp.float32),
                pltpu.VMEM((1, lanes), jnp.float32),
                pltpu.VMEM((experts, groups, lanes), jnp.float32),
                pltpu.VMEM((experts, groups, lanes), jnp.float32),
                pltpu.VMEM((chips, experts, groups, lanes), jnp.float32),
                pltpu.VMEM((experts, groups, lanes), jnp.float32),
                pltpu.VMEM((2, banks, chips, cols, lanes), jnp.float32),
                pltpu.VMEM(chunk, jnp.float32),
                pltpu.VMEM(chunk, jnp.float32),
                dma((experts + 1,)), dma((experts + 1,)), dma((2,)), dma((2,)), dma((2,)),
                regular((reach - 1,)), regular((reach - 2,)), regular, regular,
                dma((slots,)), dma((slots,)), dma(()), dma(()), dma(()), dma(()), dma(chunk[:1]), dma(chunk[:1]),
                dma(()), dma(()), dma((6,)), dma((6,)),
            ],
            compiler_params=pltpu.CompilerParams(
                collective_id=0, has_side_effects=True, vmem_limit_bytes=12 * 1024 * 1024),
            name="gather",
        )(pin(w_down), pin(avg_down), pin(router_weight.T), pin(router_gain.reshape(1, lanes)))
        big, scale, router = pl.pallas_call(
            out_kernel,
            out_shape=(
                jax.ShapeDtypeStruct(big.shape, big.dtype),
                jax.ShapeDtypeStruct(scale.shape, scale.dtype),
                jax.ShapeDtypeStruct(router.shape, router.dtype),
            ),
            in_specs=[vmem, vmem, vmem],
            out_specs=(hbm, hbm, hbm),
            scratch_shapes=[dma((experts + 2,))],
            compiler_params=pltpu.CompilerParams(vmem_limit_bytes=4 * 1024 * 1024),
            name="put_out",
        )(big, scale, router)
        return big, scale, router.T

    return jax.shard_map(
        shards,
        mesh=mesh,
        in_specs=(P("bank", None, "zero"), P("bank", None, "zero"), P("zero", "bank"), P("zero")),
        out_specs=(P("bank", None, None), P("bank", None), P()),
        check_vma=False,
    )
```

```python
import functools

import jax
import jax.numpy as jnp
from jax import lax
from jax.experimental import pallas as pl
from jax.experimental.pallas import tpu as pltpu
from jax.sharding import PartitionSpec as P

MESH = pl.DeviceIdType.MESH
SPLIT = 2
STEP, EARLY = 256, 3
SIDE = 4
PLANE = 1


def gather_kernel(
    banks, chips, w_hbm, avg_hbm, rw_hbm, gain_hbm,
    big, scale_ref, router_ref,
    wbuf, abuf, rw_ref, gain_ref, part, other, sums, total, rblk, from_l, from_r,
    wsem, asem, osem, ssem, tsem, tok_l, tok_r, tok_x, tok_z,
    rsem_r, rsem_l, send_r, send_l, esend_r, esend_l, erecv_r, erecv_l, send_p, recv_p, rsend, rrecv,
):
    experts, rows, lanes = wbuf.shape
    bank = lax.axis_index("bank")
    zero = lax.axis_index("zero")
    z = zero // 2
    core = zero % 2
    y, x = bank // SIDE, bank % SIDE
    tall = banks // SIDE
    right = {"zero": ((z + 1) % chips) * 2 + core}
    left = {"zero": ((z + chips - 1) % chips) * 2 + core}
    partner = {"zero": z * 2 + (1 - core)}
    x_up, x_down = {"bank": y * SIDE + (x + 1) % SIDE}, {"bank": y * SIDE + (x + SIDE - 1) % SIDE}
    y_up, y_down = {"bank": ((y + 1) % tall) * SIDE + x}, {"bank": ((y + tall - 1) % tall) * SIDE + x}
    groups = rows // lanes
    piece = rows // SPLIT
    chunks = experts * SPLIT
    reach = chips // 2
    ahead = EARLY * STEP
    whole_ones = ahead // piece
    rest = (ahead - whole_ones * piece) % piece
    late = chunks - whole_ones - (1 if rest else 0)

    def remote(src, dst, send, recv, to):
        return pltpu.make_async_remote_copy(src, dst, send, recv, device_id=to, device_id_type=MESH)

    def signal(sem, to):
        pl.semaphore_signal(sem, inc=1, device_id=to, device_id_type=MESH)

    small = [pltpu.make_async_copy(rw_hbm, rw_ref, asem.at[experts]),
             pltpu.make_async_copy(gain_hbm, gain_ref, wsem.at[experts])]
    loads = {}
    order = [experts - 1, *range(experts - 1)]
    for e in order:
        lw = pltpu.make_async_copy(w_hbm.at[e], wbuf.at[e], wsem.at[e])
        la = pltpu.make_async_copy(avg_hbm.at[e], abuf.at[e], asem.at[e])
        lw.start()
        la.start()
        loads[e] = (lw, la)
    for copy in small:
        copy.start()

    barrier = pltpu.get_barrier_semaphore()
    near, across = (left, right, partner), (x_up, x_down, y_up, y_down)
    for to in near:
        signal(barrier, to)

    @pl.when(z == PLANE)
    def _():
        for to in across:
            signal(barrier, to)

    eye = (
        lax.broadcasted_iota(jnp.int32, (lanes, lanes), 0)
        == lax.broadcasted_iota(jnp.int32, (lanes, lanes), 1)
    )

    def square(e):
        loads[e][0].wait()
        loads[e][1].wait()
        for g in range(groups):
            at = pl.ds(g * lanes, lanes)
            fresh = wbuf[e, at, :] + abuf[e, at, :].astype(jnp.float32)
            wbuf[e, at, :] = fresh
            row = jnp.sum(fresh * fresh, axis=1, keepdims=True)
            part[e, g:g + 1, :] = jnp.sum(jnp.where(eye, row, 0.0), axis=0, keepdims=True)

    def early_rows(p):
        at = experts * rows - ahead + p * STEP
        return at // rows, pl.ds(at % rows, STEP)

    def early_right(p):
        e, at = early_rows(p)
        return remote(wbuf.at[e, at], from_l.at[p], esend_r, erecv_r.at[p], right)

    def early_left(p):
        e, at = early_rows(p)
        return remote(wbuf.at[e, at], from_r.at[p], esend_l, erecv_l.at[p], left)

    first, second = core == 0, core == 1

    square(order[0])
    @pl.when(z == PLANE)
    def _():
        pl.semaphore_wait(barrier, len(near) + len(across))

    @pl.when(z != PLANE)
    def _():
        pl.semaphore_wait(barrier, len(near))

    signal(tok_l.at[0], right)
    signal(tok_r.at[0], left)

    @pl.when(first)
    def _():
        for p in range(EARLY):
            early_right(p).start()
            early_left(p).start()
    for e in order[1:]:
        square(e)

    swap = remote(part, other, osem.at[0], osem.at[1], partner)
    batches = [pl.ds(0, 1), pl.ds(1, experts - 1)]
    backs = [remote(total.at[at], total.at[at], tsem.at[n, 0], tsem.at[n, 1], partner) for n, at in enumerate(batches)]
    peers = [{"zero": ((z + j) % chips) * 2 + core} for j in range(1, chips)]
    peers = [to for _, to in sorted(zip(range(1, chips), peers), key=lambda p: -min(p[0], chips - p[0]))]
    most = [sums.at[pl.ds(0, chips - 1), at] for at in batches]
    fulls = [remote(ref, ref, ssem.at[n, 0], ssem.at[n, 1], partner) for n, ref in enumerate(most)]

    @pl.when(first)
    def _():
        swap.start()

    for d in range(2, reach + 1):
        pl.semaphore_wait(tok_l.at[d - 2], 1)
        if d < reach:
            signal(tok_l.at[d - 1], right)
            pl.semaphore_wait(tok_r.at[d - 2], 1)
            if d < reach - 1:
                signal(tok_r.at[d - 1], left)

    @pl.when(second)
    def _():
        swap.wait_recv()
        sums[z] = part[...] + other[...]
        for n, at in enumerate(batches):
            for to in peers:
                remote(sums.at[z, at], sums.at[z, at], ssem.at[n, 0], ssem.at[n, 1], to).start()

    @pl.when(z == PLANE)
    def _():
        for to in across:
            signal(tok_x, to)

    for copy in small:
        copy.wait()
    rblk[core, bank, z] = rw_ref[...] * gain_ref[...]

    def known(n):
        @pl.when(second)
        def _():
            fulls[n].wait_recv()
            acc = sums[0, batches[n]]
            for k in range(1, chips):
                acc = acc + sums[k, batches[n]]
            total[batches[n]] = acc
            backs[n].start()

        @pl.when(first)
        def _():
            backs[n].wait_recv()

    def place(k, src):
        return big.at[k // SPLIT, pl.ds(pl.multiple_of(k % SPLIT * piece, piece), piece),
                      pl.ds(pl.multiple_of(src * lanes, lanes), lanes)]

    def to_right(slot, k, src):
        return remote(place(k, src), place(k, src), send_r, rsem_r.at[slot], right)

    def to_left(slot, k, src):
        return remote(place(k, src), place(k, src), send_l, rsem_l.at[slot], left)

    def to_partner(k, src):
        return remote(place(k, src), place(k, src), send_p, recv_p, partner)

    def part_right(k, src):
        ref = place(k, src).at[pl.ds(0, piece - rest)]
        return remote(ref, ref, send_r, rsem_r.at[k], right)

    def part_left(k, src):
        ref = place(k, src).at[pl.ds(0, piece - rest)]
        return remote(ref, ref, send_l, rsem_l.at[k], left)

    def serve_early(src, held, p):
        e, at = early_rows(p)
        columns = pl.ds(pl.multiple_of(src * lanes, lanes), lanes)
        for j in range(STEP // lanes):
            g = at.start // lanes + j
            root = jnp.sqrt(total[e, g:g + 1, :])
            col = jnp.sum(jnp.where(eye, root, 0.0), axis=1, keepdims=True)
            big[e, g * lanes:(g + 1) * lanes, columns] = (held[p, j * lanes:(j + 1) * lanes, :] / col).astype(jnp.bfloat16)

    def serve(k, src, read):
        e = k // SPLIT
        columns = pl.ds(pl.multiple_of(src * lanes, lanes), lanes)
        for j in range(groups // SPLIT):
            g = k % SPLIT * (groups // SPLIT) + j
            at = pl.ds(pl.multiple_of(g * lanes, lanes), lanes)
            root = jnp.sqrt(total[e, pl.ds(g, 1), :])
            col = jnp.sum(jnp.where(eye, root, 0.0), axis=1, keepdims=True)
            big[e, at, columns] = (read(j) / col).astype(jnp.bfloat16)

    def own(k):
        def read(j):
            g = k % SPLIT * (groups // SPLIT) + j
            return wbuf[k // SPLIT, pl.ds(pl.multiple_of(g * lanes, lanes), lanes), :]
        serve(k, zero, read)
        to_partner(k, zero).start()

    def own_late(k, _):
        own(k)
        to_right(k, k, zero).start()
        to_left(k, k, zero).start()
        return 0

    known(0)
    lax.fori_loop(0, SPLIT, own_late, 0)
    known(1)
    lax.fori_loop(SPLIT, late, own_late, 0)

    @pl.when(second)
    def _():
        lax.fori_loop(late, chunks, own_late, 0)

    @pl.when(first)
    def _():
        for k in range(late, chunks):
            own(k)
            if rest and k == late:
                part_right(k, zero).start()
                part_left(k, zero).start()

    for e in range(experts):
        root = jnp.sqrt(total[e])
        for g in range(groups):
            scale_ref[e:e + 1, g * lanes:(g + 1) * lanes] = root[g:g + 1, :]

    from_left = [{}] + [((z + chips - d) % chips) * 2 + core for d in range(1, reach + 1)]
    from_right = [{}] + [((z + d) % chips) * 2 + core for d in range(1, reach + 1)]

    def on_right(d, slot, k):
        if d < reach - 1:
            to_right(slot + chunks, k, from_left[d]).start()
        elif d == reach - 1 and k % 2 == 0:
            to_right(d * chunks + k // 2, k, from_left[d]).start()
        to_partner(k, from_left[d]).start()

    def on_left(d, slot, k):
        if d < reach - 1:
            to_left(slot + chunks, k, from_right[d]).start()
        elif d == reach - 1 and k % 2 == 1:
            to_left(d * chunks + k // 2, k, from_right[d]).start()
        to_partner(k, from_right[d]).start()

    def pass_on(k, _):
        to_right(k, k, from_left[1]).wait_recv()
        on_right(1, k, k)
        to_left(k, k, from_right[1]).wait_recv()
        on_left(1, k, k)
        return 0

    def router_z():
        for to in peers:
            remote(rblk.at[core, bank, z], rblk.at[core, bank, z], rsend.at[0], rrecv.at[0], to).start()

    def router_wait(n, ref):
        remote(ref, ref, rsend.at[n], rrecv.at[n], partner).wait()

    def router_x():
        router_wait(0, rblk.at[core, bank, pl.ds(0, chips - 1)])

        @pl.when(z == PLANE)
        def _():
            pl.semaphore_wait(tok_x, len(across))
            for to in peers:
                signal(tok_z, to)

        @pl.when(z != PLANE)
        def _():
            pl.semaphore_wait(tok_z, 1)

        own = rblk.at[core, bank]
        remote(own, own, rsend.at[1], rrecv.at[1], x_up).start()
        remote(own, own, rsend.at[1], rrecv.at[1], x_down).start()

    def router_x2():
        router_wait(1, rblk.at[core, pl.ds(0, 2)])
        for j in range(2, SIDE - 1):
            own = rblk.at[core, y * SIDE + (x + SIDE + 1 - j) % SIDE]
            remote(own, own, rsend.at[2], rrecv.at[2], x_up).start()

    def router_y():
        router_wait(2, rblk.at[core, 0])
        own = rblk.at[core, pl.ds(y * SIDE, SIDE)]
        remote(own, own, rsend.at[3], rrecv.at[3], y_up).start()
        remote(own, own, rsend.at[3], rrecv.at[3], y_down).start()

    def router_y2():
        router_wait(3, rblk.at[core, pl.ds(0, 2 * SIDE)])
        own = rblk.at[core, pl.ds(((y + tall - 1) % tall) * SIDE, SIDE)]
        remote(own, own, rsend.at[4], rrecv.at[4], y_up).start()

    def router_partner():
        router_wait(4, rblk.at[core, pl.ds(0, SIDE)])
        remote(rblk.at[core], rblk.at[core], rsend.at[5], rrecv.at[5], partner).start()

    def router_finish():
        router_wait(5, rblk.at[core])
        for b in range(banks // 4):
            for q in range(2 * chips):
                block = jnp.concatenate([rblk[q % 2, 4 * b + i, q // 2] for i in range(4)], axis=0)
                n = block.shape[0]
                router_ref[b * n:(b + 1) * n, q * lanes:(q + 1) * lanes] = block.astype(jnp.bfloat16)

    router_steps = [router_x, router_x2, router_y, router_y2, router_partner, router_finish]
    router_z()

    @pl.when(first)
    def _():
        for p in range(EARLY):
            early_right(p).wait_recv()
            serve_early(from_left[1], from_l, p)
            early_left(p).wait_recv()
            serve_early(from_right[1], from_r, p)
        for k in range(chunks - whole_ones, chunks):
            on_right(1, k, k)
            on_left(1, k, k)

    lax.fori_loop(0, late, pass_on, 0)

    @pl.when(second)
    def _():
        lax.fori_loop(late, chunks, pass_on, 0)

    if rest:
        @pl.when(first)
        def _():
            part_right(late, from_left[1]).wait_recv()
            on_right(1, late, late)
            part_left(late, from_right[1]).wait_recv()
            on_left(1, late, late)

    router_steps.pop(0)()
    slot = chunks
    for d in range(2, reach + 1):
        last = d == reach
        for i in range(chunks // 2 if last else chunks):
            kr = 2 * i if last else i
            kl = 2 * i + 1 if last else i
            to_right(slot, kr, from_left[d]).wait_recv()
            on_right(d, slot, kr)
            to_left(slot, kl, from_right[d]).wait_recv()
            on_left(d, slot, kl)
            slot += 1
            if slot % 4 == 2 and router_steps:
                router_steps.pop(0)()

    for side in range(2):
        @pl.when(core == side)
        def _():
            if side == 0:
                swap.wait_send()
            else:
                for copy in (*fulls, *backs):
                    copy.wait_send()
            if side == 0:
                remote(from_l, from_l, esend_r, erecv_r.at[0], right).wait_send()
                remote(from_l, from_l, esend_l, erecv_l.at[0], left).wait_send()
            sent = (chunks * (chips - 1) // 2 * piece - ahead * (1 - side)) // (2 * chips)
            hops = big.at[0, pl.ds(0, sent), :]
            remote(hops, hops, send_r, rsem_r.at[0], right).wait_send()
            remote(hops, hops, send_l, rsem_l.at[0], left).wait_send()
    whole = big.at[:, :, pl.ds(0, chips * lanes)]
    remote(whole, whole, send_p, recv_p, partner).wait()


def out_kernel(big, scale, router, big_hbm, scale_hbm, router_hbm, sems):
    n = big.shape[0]
    copies = [pltpu.make_async_copy(big.at[e], big_hbm.at[e], sems.at[e]) for e in range(n)]
    copies.append(pltpu.make_async_copy(scale, scale_hbm, sems.at[n]))
    copies.append(pltpu.make_async_copy(router, router_hbm, sems.at[n + 1]))
    for copy in copies:
        copy.start()
    for copy in copies:
        copy.wait()


def solution(mesh):
    banks, zeros = mesh.shape["bank"], mesh.shape["zero"]
    chips = zeros // 2

    def shards(w_down, avg_down, router_weight, router_gain):
        experts, rows, lanes = w_down.shape
        width = lanes * zeros
        cols = router_weight.shape[1]
        vmem = pl.BlockSpec(memory_space=pltpu.VMEM)
        hbm = pl.BlockSpec(memory_space=pltpu.HBM)
        pin = lambda x: pltpu.with_memory_space_constraint(x, pltpu.HBM)
        groups = rows // lanes
        slots = experts * SPLIT * (chips - 1) // 2
        chunk = (EARLY, STEP, lanes)
        reach = chips // 2
        dma = pltpu.SemaphoreType.DMA
        regular = pltpu.SemaphoreType.REGULAR
        big, scale, router = pl.pallas_call(
            functools.partial(gather_kernel, banks, chips),
            out_shape=(
                jax.ShapeDtypeStruct((experts, rows, width), jnp.bfloat16),
                jax.ShapeDtypeStruct((experts, rows), jnp.float32),
                jax.ShapeDtypeStruct((cols * banks, width), jnp.bfloat16),
            ),
            in_specs=[hbm] * 4,
            out_specs=(vmem, vmem, vmem),
            scratch_shapes=[
                pltpu.VMEM((experts, rows, lanes), jnp.float32),
                pltpu.VMEM((experts, rows, lanes), jnp.bfloat16),
                pltpu.VMEM((cols, lanes), jnp.float32),
                pltpu.VMEM((1, lanes), jnp.float32),
                pltpu.VMEM((experts, groups, lanes), jnp.float32),
                pltpu.VMEM((experts, groups, lanes), jnp.float32),
                pltpu.VMEM((chips, experts, groups, lanes), jnp.float32),
                pltpu.VMEM((experts, groups, lanes), jnp.float32),
                pltpu.VMEM((2, banks, chips, cols, lanes), jnp.float32),
                pltpu.VMEM(chunk, jnp.float32),
                pltpu.VMEM(chunk, jnp.float32),
                dma((experts + 1,)), dma((experts + 1,)), dma((2,)), dma((2, 2)), dma((2, 2)),
                regular((reach - 1,)), regular((reach - 2,)), regular, regular,
                dma((slots,)), dma((slots,)), dma(()), dma(()), dma(()), dma(()), dma(chunk[:1]), dma(chunk[:1]),
                dma(()), dma(()), dma((6,)), dma((6,)),
            ],
            compiler_params=pltpu.CompilerParams(
                collective_id=0, has_side_effects=True, vmem_limit_bytes=12 * 1024 * 1024),
            name="gather",
        )(pin(w_down), pin(avg_down), pin(router_weight.T), pin(router_gain.reshape(1, lanes)))
        big, scale, router = pl.pallas_call(
            out_kernel,
            out_shape=(
                jax.ShapeDtypeStruct(big.shape, big.dtype),
                jax.ShapeDtypeStruct(scale.shape, scale.dtype),
                jax.ShapeDtypeStruct(router.shape, router.dtype),
            ),
            in_specs=[vmem, vmem, vmem],
            out_specs=(hbm, hbm, hbm),
            scratch_shapes=[dma((experts + 2,))],
            compiler_params=pltpu.CompilerParams(vmem_limit_bytes=4 * 1024 * 1024),
            name="put_out",
        )(big, scale, router)
        return big, scale, router.T

    return jax.shard_map(
        shards,
        mesh=mesh,
        in_specs=(P("bank", None, "zero"), P("bank", None, "zero"), P("zero", "bank"), P("zero")),
        out_specs=(P("bank", None, None), P("bank", None), P()),
        check_vma=False,
    )
```

```python
import functools

import jax
import jax.numpy as jnp
from jax import lax
from jax.experimental import pallas as pl
from jax.experimental.pallas import tpu as pltpu
from jax.sharding import PartitionSpec as P

MESH = pl.DeviceIdType.MESH
SPLIT = 2
STEP, EARLY = 256, 3
SIDE = 4
PLANE = 2


def gather_kernel(
    banks, chips, w_hbm, avg_hbm, rw_hbm, gain_hbm,
    big, scale_ref, router_ref,
    wbuf, abuf, rw_ref, gain_ref, part, other, sums, total, rblk, from_l, from_r,
    wsem, asem, osem, ssem, tsem, tok_l, tok_r, tok_x, tok_z,
    rsem_r, rsem_l, send_r, send_l, esend_r, esend_l, erecv_r, erecv_l, send_p, recv_p, rsend, rrecv,
):
    experts, rows, lanes = wbuf.shape
    bank = lax.axis_index("bank")
    zero = lax.axis_index("zero")
    z = zero // 2
    core = zero % 2
    y, x = bank // SIDE, bank % SIDE
    tall = banks // SIDE
    right = {"zero": ((z + 1) % chips) * 2 + core}
    left = {"zero": ((z + chips - 1) % chips) * 2 + core}
    partner = {"zero": z * 2 + (1 - core)}
    x_up, x_down = {"bank": y * SIDE + (x + 1) % SIDE}, {"bank": y * SIDE + (x + SIDE - 1) % SIDE}
    y_up, y_down = {"bank": ((y + 1) % tall) * SIDE + x}, {"bank": ((y + tall - 1) % tall) * SIDE + x}
    groups = rows // lanes
    piece = rows // SPLIT
    chunks = experts * SPLIT
    reach = chips // 2
    ahead = EARLY * STEP
    whole_ones = ahead // piece
    rest = (ahead - whole_ones * piece) % piece
    late = chunks - whole_ones - (1 if rest else 0)

    def remote(src, dst, send, recv, to):
        return pltpu.make_async_remote_copy(src, dst, send, recv, device_id=to, device_id_type=MESH)

    def signal(sem, to):
        pl.semaphore_signal(sem, inc=1, device_id=to, device_id_type=MESH)

    barrier = pltpu.get_barrier_semaphore()
    near, across = (left, right, partner), (x_up, x_down, y_up, y_down)
    for to in near:
        signal(barrier, to)

    @pl.when(z == PLANE)
    def _():
        for to in across:
            signal(barrier, to)

    small = [pltpu.make_async_copy(rw_hbm, rw_ref, asem.at[experts]),
             pltpu.make_async_copy(gain_hbm, gain_ref, wsem.at[experts])]
    loads = {}
    order = [experts - 1, *range(experts - 1)]
    for e in order:
        lw = pltpu.make_async_copy(w_hbm.at[e], wbuf.at[e], wsem.at[e])
        la = pltpu.make_async_copy(avg_hbm.at[e], abuf.at[e], asem.at[e])
        lw.start()
        la.start()
        loads[e] = (lw, la)
    for copy in small:
        copy.start()

    eye = (
        lax.broadcasted_iota(jnp.int32, (lanes, lanes), 0)
        == lax.broadcasted_iota(jnp.int32, (lanes, lanes), 1)
    )

    def square(e):
        loads[e][0].wait()
        loads[e][1].wait()
        for g in range(groups):
            at = pl.ds(g * lanes, lanes)
            fresh = wbuf[e, at, :] + abuf[e, at, :].astype(jnp.float32)
            wbuf[e, at, :] = fresh
            row = jnp.sum(fresh * fresh, axis=1, keepdims=True)
            part[e, g:g + 1, :] = jnp.sum(jnp.where(eye, row, 0.0), axis=0, keepdims=True)

    def early_rows(p):
        at = experts * rows - ahead + p * STEP
        return at // rows, pl.ds(at % rows, STEP)

    def early_right(p):
        e, at = early_rows(p)
        return remote(wbuf.at[e, at], from_l.at[p], esend_r, erecv_r.at[p], right)

    def early_left(p):
        e, at = early_rows(p)
        return remote(wbuf.at[e, at], from_r.at[p], esend_l, erecv_l.at[p], left)

    first, second = core == 0, core == 1

    square(order[0])
    @pl.when(z == PLANE)
    def _():
        pl.semaphore_wait(barrier, len(near) + len(across))

    @pl.when(z != PLANE)
    def _():
        pl.semaphore_wait(barrier, len(near))

    signal(tok_l.at[0], right)
    signal(tok_r.at[0], left)

    @pl.when(first)
    def _():
        for p in range(EARLY):
            early_right(p).start()
            early_left(p).start()
    for e in order[1:]:
        square(e)

    swap = remote(part, other, osem.at[0], osem.at[1], partner)
    batches = [pl.ds(0, 1), pl.ds(1, experts - 1)]
    backs = [remote(total.at[at], total.at[at], tsem.at[n, 0], tsem.at[n, 1], partner) for n, at in enumerate(batches)]
    peers = [{"zero": ((z + j) % chips) * 2 + core} for j in range(1, chips)]
    peers = [to for _, to in sorted(zip(range(1, chips), peers), key=lambda p: -min(p[0], chips - p[0]))]
    most = [sums.at[pl.ds(0, chips - 1), at] for at in batches]
    fulls = [remote(ref, ref, ssem.at[n, 0], ssem.at[n, 1], partner) for n, ref in enumerate(most)]

    @pl.when(first)
    def _():
        swap.start()

    for d in range(2, reach + 1):
        pl.semaphore_wait(tok_l.at[d - 2], 1)
        if d < reach:
            signal(tok_l.at[d - 1], right)
            pl.semaphore_wait(tok_r.at[d - 2], 1)
            if d < reach - 1:
                signal(tok_r.at[d - 1], left)

    @pl.when(second)
    def _():
        swap.wait_recv()
        sums[z] = part[...] + other[...]
        for n, at in enumerate(batches):
            for to in peers:
                remote(sums.at[z, at], sums.at[z, at], ssem.at[n, 0], ssem.at[n, 1], to).start()

    @pl.when(z == PLANE)
    def _():
        for to in across:
            signal(tok_x, to)

    for copy in small:
        copy.wait()
    rblk[core, bank, z] = rw_ref[...] * gain_ref[...]

    def known(n):
        @pl.when(second)
        def _():
            fulls[n].wait_recv()
            acc = sums[0, batches[n]]
            for k in range(1, chips):
                acc = acc + sums[k, batches[n]]
            total[batches[n]] = acc
            backs[n].start()

        @pl.when(first)
        def _():
            backs[n].wait_recv()

    def place(k, src):
        return big.at[k // SPLIT, pl.ds(pl.multiple_of(k % SPLIT * piece, piece), piece),
                      pl.ds(pl.multiple_of(src * lanes, lanes), lanes)]

    def to_right(slot, k, src):
        return remote(place(k, src), place(k, src), send_r, rsem_r.at[slot], right)

    def to_left(slot, k, src):
        return remote(place(k, src), place(k, src), send_l, rsem_l.at[slot], left)

    def to_partner(k, src):
        return remote(place(k, src), place(k, src), send_p, recv_p, partner)

    def part_right(k, src):
        ref = place(k, src).at[pl.ds(0, piece - rest)]
        return remote(ref, ref, send_r, rsem_r.at[k], right)

    def part_left(k, src):
        ref = place(k, src).at[pl.ds(0, piece - rest)]
        return remote(ref, ref, send_l, rsem_l.at[k], left)

    def serve_early(src, held, p):
        e, at = early_rows(p)
        columns = pl.ds(pl.multiple_of(src * lanes, lanes), lanes)
        for j in range(STEP // lanes):
            g = at.start // lanes + j
            root = jnp.sqrt(total[e, g:g + 1, :])
            col = jnp.sum(jnp.where(eye, root, 0.0), axis=1, keepdims=True)
            big[e, g * lanes:(g + 1) * lanes, columns] = (held[p, j * lanes:(j + 1) * lanes, :] / col).astype(jnp.bfloat16)

    def serve(k, src, read):
        e = k // SPLIT
        columns = pl.ds(pl.multiple_of(src * lanes, lanes), lanes)
        for j in range(groups // SPLIT):
            g = k % SPLIT * (groups // SPLIT) + j
            at = pl.ds(pl.multiple_of(g * lanes, lanes), lanes)
            root = jnp.sqrt(total[e, pl.ds(g, 1), :])
            col = jnp.sum(jnp.where(eye, root, 0.0), axis=1, keepdims=True)
            big[e, at, columns] = (read(j) / col).astype(jnp.bfloat16)

    def own(k):
        def read(j):
            g = k % SPLIT * (groups // SPLIT) + j
            return wbuf[k // SPLIT, pl.ds(pl.multiple_of(g * lanes, lanes), lanes), :]
        serve(k, zero, read)
        to_partner(k, zero).start()

    def own_late(k, _):
        own(k)
        to_right(k, k, zero).start()
        to_left(k, k, zero).start()
        return 0

    known(0)
    lax.fori_loop(0, SPLIT, own_late, 0)
    known(1)
    lax.fori_loop(SPLIT, late, own_late, 0)

    @pl.when(second)
    def _():
        lax.fori_loop(late, chunks, own_late, 0)

    @pl.when(first)
    def _():
        for k in range(late, chunks):
            own(k)
            if rest and k == late:
                part_right(k, zero).start()
                part_left(k, zero).start()

    for e in range(experts):
        root = jnp.sqrt(total[e])
        for g in range(groups):
            scale_ref[e:e + 1, g * lanes:(g + 1) * lanes] = root[g:g + 1, :]

    from_left = [{}] + [((z + chips - d) % chips) * 2 + core for d in range(1, reach + 1)]
    from_right = [{}] + [((z + d) % chips) * 2 + core for d in range(1, reach + 1)]

    def on_right(d, slot, k):
        if d < reach - 1:
            to_right(slot + chunks, k, from_left[d]).start()
        elif d == reach - 1 and k % 2 == 0:
            to_right(d * chunks + k // 2, k, from_left[d]).start()
        to_partner(k, from_left[d]).start()

    def on_left(d, slot, k):
        if d < reach - 1:
            to_left(slot + chunks, k, from_right[d]).start()
        elif d == reach - 1 and k % 2 == 1:
            to_left(d * chunks + k // 2, k, from_right[d]).start()
        to_partner(k, from_right[d]).start()

    def pass_on(k, _):
        to_right(k, k, from_left[1]).wait_recv()
        on_right(1, k, k)
        to_left(k, k, from_right[1]).wait_recv()
        on_left(1, k, k)
        return 0

    def router_z():
        for to in peers:
            remote(rblk.at[core, bank, z], rblk.at[core, bank, z], rsend.at[0], rrecv.at[0], to).start()

    def router_wait(n, ref):
        remote(ref, ref, rsend.at[n], rrecv.at[n], partner).wait()

    def router_x():
        router_wait(0, rblk.at[core, bank, pl.ds(0, chips - 1)])

        @pl.when(z == PLANE)
        def _():
            pl.semaphore_wait(tok_x, len(across))
            for to in peers:
                signal(tok_z, to)

        @pl.when(z != PLANE)
        def _():
            pl.semaphore_wait(tok_z, 1)

        own = rblk.at[core, bank]
        remote(own, own, rsend.at[1], rrecv.at[1], x_up).start()
        remote(own, own, rsend.at[1], rrecv.at[1], x_down).start()

    def router_x2():
        router_wait(1, rblk.at[core, pl.ds(0, 2)])
        for j in range(2, SIDE - 1):
            own = rblk.at[core, y * SIDE + (x + SIDE + 1 - j) % SIDE]
            remote(own, own, rsend.at[2], rrecv.at[2], x_up).start()

    def router_y():
        router_wait(2, rblk.at[core, 0])
        own = rblk.at[core, pl.ds(y * SIDE, SIDE)]
        remote(own, own, rsend.at[3], rrecv.at[3], y_up).start()
        remote(own, own, rsend.at[3], rrecv.at[3], y_down).start()

    def router_y2():
        router_wait(3, rblk.at[core, pl.ds(0, 2 * SIDE)])
        own = rblk.at[core, pl.ds(((y + tall - 1) % tall) * SIDE, SIDE)]
        remote(own, own, rsend.at[4], rrecv.at[4], y_up).start()

    def router_partner():
        router_wait(4, rblk.at[core, pl.ds(0, SIDE)])
        remote(rblk.at[core], rblk.at[core], rsend.at[5], rrecv.at[5], partner).start()

    def router_finish():
        router_wait(5, rblk.at[core])
        for b in range(banks // 4):
            for q in range(2 * chips):
                block = jnp.concatenate([rblk[q % 2, 4 * b + i, q // 2] for i in range(4)], axis=0)
                n = block.shape[0]
                router_ref[b * n:(b + 1) * n, q * lanes:(q + 1) * lanes] = block.astype(jnp.bfloat16)

    router_steps = [router_x, router_x2, router_y, router_y2, router_partner, router_finish]
    router_z()

    @pl.when(first)
    def _():
        for p in range(EARLY):
            early_right(p).wait_recv()
            serve_early(from_left[1], from_l, p)
            early_left(p).wait_recv()
            serve_early(from_right[1], from_r, p)
        for k in range(chunks - whole_ones, chunks):
            on_right(1, k, k)
            on_left(1, k, k)

    lax.fori_loop(0, late, pass_on, 0)

    @pl.when(second)
    def _():
        lax.fori_loop(late, chunks, pass_on, 0)

    if rest:
        @pl.when(first)
        def _():
            part_right(late, from_left[1]).wait_recv()
            on_right(1, late, late)
            part_left(late, from_right[1]).wait_recv()
            on_left(1, late, late)

    router_steps.pop(0)()
    slot = chunks
    for d in range(2, reach + 1):
        last = d == reach
        for i in range(chunks // 2 if last else chunks):
            kr = 2 * i if last else i
            kl = 2 * i + 1 if last else i
            to_right(slot, kr, from_left[d]).wait_recv()
            on_right(d, slot, kr)
            to_left(slot, kl, from_right[d]).wait_recv()
            on_left(d, slot, kl)
            slot += 1
            if slot % 4 == 2 and router_steps:
                router_steps.pop(0)()

    for side in range(2):
        @pl.when(core == side)
        def _():
            if side == 0:
                swap.wait_send()
            else:
                for copy in (*fulls, *backs):
                    copy.wait_send()
            if side == 0:
                remote(from_l, from_l, esend_r, erecv_r.at[0], right).wait_send()
                remote(from_l, from_l, esend_l, erecv_l.at[0], left).wait_send()
            sent = (chunks * (chips - 1) // 2 * piece - ahead * (1 - side)) // (2 * chips)
            hops = big.at[0, pl.ds(0, sent), :]
            remote(hops, hops, send_r, rsem_r.at[0], right).wait_send()
            remote(hops, hops, send_l, rsem_l.at[0], left).wait_send()
    whole = big.at[:, :, pl.ds(0, chips * lanes)]
    remote(whole, whole, send_p, recv_p, partner).wait()


def out_kernel(big, scale, router, big_hbm, scale_hbm, router_hbm, sems):
    n = big.shape[0]
    copies = [pltpu.make_async_copy(big.at[e], big_hbm.at[e], sems.at[e]) for e in range(n)]
    copies.append(pltpu.make_async_copy(scale, scale_hbm, sems.at[n]))
    copies.append(pltpu.make_async_copy(router, router_hbm, sems.at[n + 1]))
    for copy in copies:
        copy.start()
    for copy in copies:
        copy.wait()


def solution(mesh):
    banks, zeros = mesh.shape["bank"], mesh.shape["zero"]
    chips = zeros // 2

    def shards(w_down, avg_down, router_weight, router_gain):
        experts, rows, lanes = w_down.shape
        width = lanes * zeros
        cols = router_weight.shape[1]
        vmem = pl.BlockSpec(memory_space=pltpu.VMEM)
        hbm = pl.BlockSpec(memory_space=pltpu.HBM)
        pin = lambda x: pltpu.with_memory_space_constraint(x, pltpu.HBM)
        groups = rows // lanes
        slots = experts * SPLIT * (chips - 1) // 2
        chunk = (EARLY, STEP, lanes)
        reach = chips // 2
        dma = pltpu.SemaphoreType.DMA
        regular = pltpu.SemaphoreType.REGULAR
        big, scale, router = pl.pallas_call(
            functools.partial(gather_kernel, banks, chips),
            out_shape=(
                jax.ShapeDtypeStruct((experts, rows, width), jnp.bfloat16),
                jax.ShapeDtypeStruct((experts, rows), jnp.float32),
                jax.ShapeDtypeStruct((cols * banks, width), jnp.bfloat16),
            ),
            in_specs=[hbm] * 4,
            out_specs=(vmem, vmem, vmem),
            scratch_shapes=[
                pltpu.VMEM((experts, rows, lanes), jnp.float32),
                pltpu.VMEM((experts, rows, lanes), jnp.bfloat16),
                pltpu.VMEM((cols, lanes), jnp.float32),
                pltpu.VMEM((1, lanes), jnp.float32),
                pltpu.VMEM((experts, groups, lanes), jnp.float32),
                pltpu.VMEM((experts, groups, lanes), jnp.float32),
                pltpu.VMEM((chips, experts, groups, lanes), jnp.float32),
                pltpu.VMEM((experts, groups, lanes), jnp.float32),
                pltpu.VMEM((2, banks, chips, cols, lanes), jnp.float32),
                pltpu.VMEM(chunk, jnp.float32),
                pltpu.VMEM(chunk, jnp.float32),
                dma((experts + 1,)), dma((experts + 1,)), dma((2,)), dma((2, 2)), dma((2, 2)),
                regular((reach - 1,)), regular((reach - 2,)), regular, regular,
                dma((slots,)), dma((slots,)), dma(()), dma(()), dma(()), dma(()), dma(chunk[:1]), dma(chunk[:1]),
                dma(()), dma(()), dma((6,)), dma((6,)),
            ],
            compiler_params=pltpu.CompilerParams(
                collective_id=0, has_side_effects=True, vmem_limit_bytes=12 * 1024 * 1024),
            name="gather",
        )(pin(w_down), pin(avg_down), pin(router_weight.T), pin(router_gain.reshape(1, lanes)))
        big, scale, router = pl.pallas_call(
            out_kernel,
            out_shape=(
                jax.ShapeDtypeStruct(big.shape, big.dtype),
                jax.ShapeDtypeStruct(scale.shape, scale.dtype),
                jax.ShapeDtypeStruct(router.shape, router.dtype),
            ),
            in_specs=[vmem, vmem, vmem],
            out_specs=(hbm, hbm, hbm),
            scratch_shapes=[dma((experts + 2,))],
            compiler_params=pltpu.CompilerParams(vmem_limit_bytes=4 * 1024 * 1024),
            name="put_out",
        )(big, scale, router)
        return big, scale, router.T

    return jax.shard_map(
        shards,
        mesh=mesh,
        in_specs=(P("bank", None, "zero"), P("bank", None, "zero"), P("zero", "bank"), P("zero")),
        out_specs=(P("bank", None, None), P("bank", None), P()),
        check_vma=False,
    )
```

```python
import functools

import jax
import jax.numpy as jnp
from jax import lax
from jax.experimental import pallas as pl
from jax.experimental.pallas import tpu as pltpu
from jax.sharding import PartitionSpec as P

MESH = pl.DeviceIdType.MESH
SPLIT = 2
STEP, EARLY = 256, 3
SIDE = 4
PLANE = 2


def gather_kernel(
    banks, chips, w_hbm, avg_hbm, rw_hbm, gain_hbm,
    big, scale_ref, router_ref,
    wbuf, abuf, rw_ref, gain_ref, part, other, sums, total, rblk, from_l, from_r,
    wsem, asem, osem, ssem, tsem, tok_l, tok_r, tok_x, tok_z,
    rsem_r, rsem_l, send_r, send_l, esend_r, esend_l, erecv_r, erecv_l, send_p, recv_p, rsend, rrecv,
):
    experts, rows, lanes = wbuf.shape
    bank = lax.axis_index("bank")
    zero = lax.axis_index("zero")
    z = zero // 2
    core = zero % 2
    y, x = bank // SIDE, bank % SIDE
    tall = banks // SIDE
    right = {"zero": ((z + 1) % chips) * 2 + core}
    left = {"zero": ((z + chips - 1) % chips) * 2 + core}
    partner = {"zero": z * 2 + (1 - core)}
    x_up, x_down = {"bank": y * SIDE + (x + 1) % SIDE}, {"bank": y * SIDE + (x + SIDE - 1) % SIDE}
    y_up, y_down = {"bank": ((y + 1) % tall) * SIDE + x}, {"bank": ((y + tall - 1) % tall) * SIDE + x}
    groups = rows // lanes
    piece = rows // SPLIT
    chunks = experts * SPLIT
    reach = chips // 2
    ahead = EARLY * STEP
    whole_ones = ahead // piece
    rest = (ahead - whole_ones * piece) % piece
    late = chunks - whole_ones - (1 if rest else 0)

    def remote(src, dst, send, recv, to):
        return pltpu.make_async_remote_copy(src, dst, send, recv, device_id=to, device_id_type=MESH)

    def signal(sem, to):
        pl.semaphore_signal(sem, inc=1, device_id=to, device_id_type=MESH)

    small = [pltpu.make_async_copy(rw_hbm, rw_ref, asem.at[experts]),
             pltpu.make_async_copy(gain_hbm, gain_ref, wsem.at[experts])]
    loads = {}
    order = [experts - 1, *range(experts - 1)]
    for e in order:
        lw = pltpu.make_async_copy(w_hbm.at[e], wbuf.at[e], wsem.at[e])
        la = pltpu.make_async_copy(avg_hbm.at[e], abuf.at[e], asem.at[e])
        lw.start()
        la.start()
        loads[e] = (lw, la)
    for copy in small:
        copy.start()

    barrier = pltpu.get_barrier_semaphore()
    near, across = (left, right, partner), (x_up, x_down, y_up, y_down)
    for to in near:
        signal(barrier, to)

    @pl.when(z == PLANE)
    def _():
        for to in across:
            signal(barrier, to)

    eye = (
        lax.broadcasted_iota(jnp.int32, (lanes, lanes), 0)
        == lax.broadcasted_iota(jnp.int32, (lanes, lanes), 1)
    )

    def square(e):
        loads[e][0].wait()
        loads[e][1].wait()
        for g in range(groups):
            at = pl.ds(g * lanes, lanes)
            fresh = wbuf[e, at, :] + abuf[e, at, :].astype(jnp.float32)
            wbuf[e, at, :] = fresh
            row = jnp.sum(fresh * fresh, axis=1, keepdims=True)
            part[e, g:g + 1, :] = jnp.sum(jnp.where(eye, row, 0.0), axis=0, keepdims=True)

    def early_rows(p):
        at = experts * rows - ahead + p * STEP
        return at // rows, pl.ds(at % rows, STEP)

    def early_right(p):
        e, at = early_rows(p)
        return remote(wbuf.at[e, at], from_l.at[p], esend_r, erecv_r.at[p], right)

    def early_left(p):
        e, at = early_rows(p)
        return remote(wbuf.at[e, at], from_r.at[p], esend_l, erecv_l.at[p], left)

    first, second = core == 0, core == 1

    square(order[0])
    @pl.when(z == PLANE)
    def _():
        pl.semaphore_wait(barrier, len(near) + len(across))

    @pl.when(z != PLANE)
    def _():
        pl.semaphore_wait(barrier, len(near))

    signal(tok_l.at[0], right)
    signal(tok_r.at[0], left)

    @pl.when(first)
    def _():
        for p in range(EARLY):
            early_right(p).start()
            early_left(p).start()
    for e in order[1:]:
        square(e)

    swap = remote(part, other, osem.at[0], osem.at[1], partner)
    batches = [pl.ds(0, 1), pl.ds(1, experts - 1)]
    backs = [remote(total.at[at], total.at[at], tsem.at[n, 0], tsem.at[n, 1], partner) for n, at in enumerate(batches)]
    peers = [{"zero": ((z + j) % chips) * 2 + core} for j in range(1, chips)]
    peers = [to for _, to in sorted(zip(range(1, chips), peers), key=lambda p: -min(p[0], chips - p[0]))]
    most = [sums.at[pl.ds(0, chips - 1), at] for at in batches]
    fulls = [remote(ref, ref, ssem.at[n, 0], ssem.at[n, 1], partner) for n, ref in enumerate(most)]

    @pl.when(first)
    def _():
        swap.start()

    for d in range(2, reach + 1):
        pl.semaphore_wait(tok_l.at[d - 2], 1)
        if d < reach:
            signal(tok_l.at[d - 1], right)
            pl.semaphore_wait(tok_r.at[d - 2], 1)
            if d < reach - 1:
                signal(tok_r.at[d - 1], left)

    @pl.when(second)
    def _():
        swap.wait_recv()
        sums[z] = part[...] + other[...]
        for n, at in enumerate(batches):
            for to in peers:
                remote(sums.at[z, at], sums.at[z, at], ssem.at[n, 0], ssem.at[n, 1], to).start()

    @pl.when(z == PLANE)
    def _():
        for to in across:
            signal(tok_x, to)

    for copy in small:
        copy.wait()
    rblk[core, bank, z] = rw_ref[...] * gain_ref[...]

    def known(n):
        @pl.when(second)
        def _():
            fulls[n].wait_recv()
            acc = sums[0, batches[n]]
            for k in range(1, chips):
                acc = acc + sums[k, batches[n]]
            total[batches[n]] = acc
            backs[n].start()

        @pl.when(first)
        def _():
            backs[n].wait_recv()

    def place(k, src):
        return big.at[k // SPLIT, pl.ds(pl.multiple_of(k % SPLIT * piece, piece), piece),
                      pl.ds(pl.multiple_of(src * lanes, lanes), lanes)]

    def to_right(slot, k, src):
        return remote(place(k, src), place(k, src), send_r, rsem_r.at[slot], right)

    def to_left(slot, k, src):
        return remote(place(k, src), place(k, src), send_l, rsem_l.at[slot], left)

    def to_partner(k, src):
        return remote(place(k, src), place(k, src), send_p, recv_p, partner)

    def part_right(k, src):
        ref = place(k, src).at[pl.ds(0, piece - rest)]
        return remote(ref, ref, send_r, rsem_r.at[k], right)

    def part_left(k, src):
        ref = place(k, src).at[pl.ds(0, piece - rest)]
        return remote(ref, ref, send_l, rsem_l.at[k], left)

    def serve_early(src, held, p):
        e, at = early_rows(p)
        columns = pl.ds(pl.multiple_of(src * lanes, lanes), lanes)
        for j in range(STEP // lanes):
            g = at.start // lanes + j
            root = jnp.sqrt(total[e, g:g + 1, :])
            col = jnp.sum(jnp.where(eye, root, 0.0), axis=1, keepdims=True)
            big[e, g * lanes:(g + 1) * lanes, columns] = (held[p, j * lanes:(j + 1) * lanes, :] / col).astype(jnp.bfloat16)

    def serve(k, src, read):
        e = k // SPLIT
        columns = pl.ds(pl.multiple_of(src * lanes, lanes), lanes)
        for j in range(groups // SPLIT):
            g = k % SPLIT * (groups // SPLIT) + j
            at = pl.ds(pl.multiple_of(g * lanes, lanes), lanes)
            root = jnp.sqrt(total[e, pl.ds(g, 1), :])
            col = jnp.sum(jnp.where(eye, root, 0.0), axis=1, keepdims=True)
            big[e, at, columns] = (read(j) / col).astype(jnp.bfloat16)

    def own(k):
        def read(j):
            g = k % SPLIT * (groups // SPLIT) + j
            return wbuf[k // SPLIT, pl.ds(pl.multiple_of(g * lanes, lanes), lanes), :]
        serve(k, zero, read)
        to_partner(k, zero).start()

    def own_late(k, _):
        own(k)
        to_right(k, k, zero).start()
        to_left(k, k, zero).start()
        return 0

    known(0)
    lax.fori_loop(0, SPLIT, own_late, 0)
    known(1)
    lax.fori_loop(SPLIT, late, own_late, 0)

    @pl.when(second)
    def _():
        lax.fori_loop(late, chunks, own_late, 0)

    @pl.when(first)
    def _():
        for k in range(late, chunks):
            own(k)
            if rest and k == late:
                part_right(k, zero).start()
                part_left(k, zero).start()

    for e in range(experts):
        root = jnp.sqrt(total[e])
        for g in range(groups):
            scale_ref[e:e + 1, g * lanes:(g + 1) * lanes] = root[g:g + 1, :]

    from_left = [{}] + [((z + chips - d) % chips) * 2 + core for d in range(1, reach + 1)]
    from_right = [{}] + [((z + d) % chips) * 2 + core for d in range(1, reach + 1)]

    def on_right(d, slot, k):
        if d < reach - 1:
            to_right(slot + chunks, k, from_left[d]).start()
        elif d == reach - 1 and k % 2 == 0:
            to_right(d * chunks + k // 2, k, from_left[d]).start()
        to_partner(k, from_left[d]).start()

    def on_left(d, slot, k):
        if d < reach - 1:
            to_left(slot + chunks, k, from_right[d]).start()
        elif d == reach - 1 and k % 2 == 1:
            to_left(d * chunks + k // 2, k, from_right[d]).start()
        to_partner(k, from_right[d]).start()

    def pass_on(k, _):
        to_right(k, k, from_left[1]).wait_recv()
        on_right(1, k, k)
        to_left(k, k, from_right[1]).wait_recv()
        on_left(1, k, k)
        return 0

    def router_z():
        for to in peers:
            remote(rblk.at[core, bank, z], rblk.at[core, bank, z], rsend.at[0], rrecv.at[0], to).start()

    def router_wait(n, ref):
        remote(ref, ref, rsend.at[n], rrecv.at[n], partner).wait()

    def router_x():
        router_wait(0, rblk.at[core, bank, pl.ds(0, chips - 1)])

        @pl.when(z == PLANE)
        def _():
            pl.semaphore_wait(tok_x, len(across))
            for to in peers:
                signal(tok_z, to)

        @pl.when(z != PLANE)
        def _():
            pl.semaphore_wait(tok_z, 1)

        own = rblk.at[core, bank]
        remote(own, own, rsend.at[1], rrecv.at[1], x_up).start()
        remote(own, own, rsend.at[1], rrecv.at[1], x_down).start()

    def router_x2():
        router_wait(1, rblk.at[core, pl.ds(0, 2)])
        for j in range(2, SIDE - 1):
            own = rblk.at[core, y * SIDE + (x + SIDE + 1 - j) % SIDE]
            remote(own, own, rsend.at[2], rrecv.at[2], x_up).start()

    def router_y():
        router_wait(2, rblk.at[core, 0])
        own = rblk.at[core, pl.ds(y * SIDE, SIDE)]
        remote(own, own, rsend.at[3], rrecv.at[3], y_up).start()
        remote(own, own, rsend.at[3], rrecv.at[3], y_down).start()

    def router_y2():
        router_wait(3, rblk.at[core, pl.ds(0, 2 * SIDE)])
        own = rblk.at[core, pl.ds(((y + tall - 1) % tall) * SIDE, SIDE)]
        remote(own, own, rsend.at[4], rrecv.at[4], y_up).start()

    def router_partner():
        router_wait(4, rblk.at[core, pl.ds(0, SIDE)])
        remote(rblk.at[core], rblk.at[core], rsend.at[5], rrecv.at[5], partner).start()

    def router_finish():
        router_wait(5, rblk.at[core])
        for b in range(banks // 4):
            for q in range(2 * chips):
                block = jnp.concatenate([rblk[q % 2, 4 * b + i, q // 2] for i in range(4)], axis=0)
                n = block.shape[0]
                router_ref[b * n:(b + 1) * n, q * lanes:(q + 1) * lanes] = block.astype(jnp.bfloat16)

    router_steps = [router_x, router_x2, router_y, router_y2, router_partner, router_finish]
    router_z()

    @pl.when(first)
    def _():
        for p in range(EARLY):
            early_right(p).wait_recv()
            serve_early(from_left[1], from_l, p)
            early_left(p).wait_recv()
            serve_early(from_right[1], from_r, p)
        for k in range(chunks - whole_ones, chunks):
            on_right(1, k, k)
            on_left(1, k, k)

    lax.fori_loop(0, late, pass_on, 0)

    @pl.when(second)
    def _():
        lax.fori_loop(late, chunks, pass_on, 0)

    if rest:
        @pl.when(first)
        def _():
            part_right(late, from_left[1]).wait_recv()
            on_right(1, late, late)
            part_left(late, from_right[1]).wait_recv()
            on_left(1, late, late)

    router_steps.pop(0)()
    slot = chunks
    for d in range(2, reach + 1):
        last = d == reach
        for i in range(chunks // 2 if last else chunks):
            kr = 2 * i if last else i
            kl = 2 * i + 1 if last else i
            to_right(slot, kr, from_left[d]).wait_recv()
            on_right(d, slot, kr)
            to_left(slot, kl, from_right[d]).wait_recv()
            on_left(d, slot, kl)
            slot += 1
            if slot % 4 == 2 and router_steps:
                router_steps.pop(0)()

    for side in range(2):
        @pl.when(core == side)
        def _():
            if side == 0:
                swap.wait_send()
            else:
                for copy in (*fulls, *backs):
                    copy.wait_send()
            if side == 0:
                remote(from_l, from_l, esend_r, erecv_r.at[0], right).wait_send()
                remote(from_l, from_l, esend_l, erecv_l.at[0], left).wait_send()
            sent = (chunks * (chips - 1) // 2 * piece - ahead * (1 - side)) // (2 * chips)
            hops = big.at[0, pl.ds(0, sent), :]
            remote(hops, hops, send_r, rsem_r.at[0], right).wait_send()
            remote(hops, hops, send_l, rsem_l.at[0], left).wait_send()
    whole = big.at[:, :, pl.ds(0, chips * lanes)]
    remote(whole, whole, send_p, recv_p, partner).wait()


def out_kernel(big, scale, router, big_hbm, scale_hbm, router_hbm, sems):
    n = big.shape[0]
    copies = [pltpu.make_async_copy(big.at[e], big_hbm.at[e], sems.at[e]) for e in range(n)]
    copies.append(pltpu.make_async_copy(scale, scale_hbm, sems.at[n]))
    copies.append(pltpu.make_async_copy(router, router_hbm, sems.at[n + 1]))
    for copy in copies:
        copy.start()
    for copy in copies:
        copy.wait()


def solution(mesh):
    banks, zeros = mesh.shape["bank"], mesh.shape["zero"]
    chips = zeros // 2

    def shards(w_down, avg_down, router_weight, router_gain):
        experts, rows, lanes = w_down.shape
        width = lanes * zeros
        cols = router_weight.shape[1]
        vmem = pl.BlockSpec(memory_space=pltpu.VMEM)
        hbm = pl.BlockSpec(memory_space=pltpu.HBM)
        pin = lambda x: pltpu.with_memory_space_constraint(x, pltpu.HBM)
        groups = rows // lanes
        slots = experts * SPLIT * (chips - 1) // 2
        chunk = (EARLY, STEP, lanes)
        reach = chips // 2
        dma = pltpu.SemaphoreType.DMA
        regular = pltpu.SemaphoreType.REGULAR
        big, scale, router = pl.pallas_call(
            functools.partial(gather_kernel, banks, chips),
            out_shape=(
                jax.ShapeDtypeStruct((experts, rows, width), jnp.bfloat16),
                jax.ShapeDtypeStruct((experts, rows), jnp.float32),
                jax.ShapeDtypeStruct((cols * banks, width), jnp.bfloat16),
            ),
            in_specs=[hbm] * 4,
            out_specs=(vmem, vmem, vmem),
            scratch_shapes=[
                pltpu.VMEM((experts, rows, lanes), jnp.float32),
                pltpu.VMEM((experts, rows, lanes), jnp.bfloat16),
                pltpu.VMEM((cols, lanes), jnp.float32),
                pltpu.VMEM((1, lanes), jnp.float32),
                pltpu.VMEM((experts, groups, lanes), jnp.float32),
                pltpu.VMEM((experts, groups, lanes), jnp.float32),
                pltpu.VMEM((chips, experts, groups, lanes), jnp.float32),
                pltpu.VMEM((experts, groups, lanes), jnp.float32),
                pltpu.VMEM((2, banks, chips, cols, lanes), jnp.float32),
                pltpu.VMEM(chunk, jnp.float32),
                pltpu.VMEM(chunk, jnp.float32),
                dma((experts + 1,)), dma((experts + 1,)), dma((2,)), dma((2, 2)), dma((2, 2)),
                regular((reach - 1,)), regular((reach - 2,)), regular, regular,
                dma((slots,)), dma((slots,)), dma(()), dma(()), dma(()), dma(()), dma(chunk[:1]), dma(chunk[:1]),
                dma(()), dma(()), dma((6,)), dma((6,)),
            ],
            compiler_params=pltpu.CompilerParams(
                collective_id=0, has_side_effects=True, vmem_limit_bytes=12 * 1024 * 1024),
            name="gather",
        )(pin(w_down), pin(avg_down), pin(router_weight.T), pin(router_gain.reshape(1, lanes)))
        big, scale, router = pl.pallas_call(
            out_kernel,
            out_shape=(
                jax.ShapeDtypeStruct(big.shape, big.dtype),
                jax.ShapeDtypeStruct(scale.shape, scale.dtype),
                jax.ShapeDtypeStruct(router.shape, router.dtype),
            ),
            in_specs=[vmem, vmem, vmem],
            out_specs=(hbm, hbm, hbm),
            scratch_shapes=[dma((experts + 2,))],
            compiler_params=pltpu.CompilerParams(vmem_limit_bytes=4 * 1024 * 1024),
            name="put_out",
        )(big, scale, router)
        return big, scale, router.T

    return jax.shard_map(
        shards,
        mesh=mesh,
        in_specs=(P("bank", None, "zero"), P("bank", None, "zero"), P("zero", "bank"), P("zero")),
        out_specs=(P("bank", None, None), P("bank", None), P()),
        check_vma=False,
    )
```
